32 devices in a mesh: pair: 8 (over z, x), sector: 4 (over y, core).
Axes of the slice: x: 2, y: 2, z: 4, core: 2. Of those that a mesh axis runs over, the one named last changes fastest.
Arguments:
- wave: bfloat16 [4, 1024, 1024], P('sector', 'pair'), may hold values from -6 to 6
- left_ops: bfloat16 [16, 4, 1024, 1024], P('pair', 'sector'), may hold values from -0.1875 to 0.1875
- right_ops: bfloat16 [16, 4, 1024, 1024], P('pair', 'sector'), may hold values from -0.046875 to 0.046875
- targets: int32 [16, 4], P('pair', 'sector'), may hold values from -1 to 3
- sector_sizes: int32 [4], replicated, may hold values from 256 to 1024
- pair_ids: int32 [16], P('pair'), may hold values from 0 to 15, each once
- pair_coefficients: float32 [16], replicated, may hold values from 0.25 to 2
Outputs:
- sigma_blocks: float32 [4, 1024, 1024], P('sector', 'pair')
The draws below stay inside these ranges and needn't reach their ends.
Inputs may be any that keep to these rules, and one draw needn't show every extreme that they name: `pair_ids`: each orbital pair once.
All inputs are finite; a program needn't handle non-finite values.
Results may differ from the reference program's by a relative error of at most 0.0029.
Values may be sent and summed in bfloat16 or wider, within the bound.
A program may use at most 128 MiB of HBM per device.

```python
import math
import jax
import jax.numpy as jnp
from jax import lax

BLOCK = 1024
SECTORS = 4
PAIRS = 16


def set_ends(values, own_key, low, largest):
    longest = values.shape.index(max(values.shape))
    spots = []
    for shift in (0, 1):
        where = [jax.random.randint(jax.random.fold_in(own_key, axis), (), 0, length) for axis, length in enumerate(values.shape)]
        where[longest] = (where[longest] + shift) % values.shape[longest]
        spots.append(tuple(where))
    return values.at[spots[0]].set(low).at[spots[1]].set(largest)


def levels(key, dims, cuts, low, top_value):
    gain = 1.0
    for axis_at, parts in cuts:
        heights = jax.random.uniform(jax.random.fold_in(jax.random.fold_in(key, 6), axis_at), (parts,), jnp.float32, low / len(cuts), top_value / len(cuts))
        gain = gain * jnp.repeat(jnp.exp(heights), dims[axis_at] // parts).reshape((-1,) + (1,) * (len(dims) - 1 - axis_at))
    return gain


def normal_values(rng, shape, deviation, reach, shards=(), held_as=jnp.bfloat16):
    level = levels(rng, shape, shards, -0.22, 0.18) if shards else 1.0
    values = jax.random.normal(rng, shape, jnp.float32) * deviation * level
    return jnp.minimum(jnp.maximum(values, -reach), reach).astype(held_as)


def setup_inputs(seed: int = 0) -> dict:
    arg_keys = jax.random.split(jax.random.key(seed), 8)
    return {
        "wave": normal_values(arg_keys[0], (SECTORS, BLOCK, BLOCK), 1.0, 6.0, ((0, 4), (1, 8))),
        "left_ops": normal_values(arg_keys[1], (PAIRS, SECTORS, BLOCK, BLOCK), BLOCK ** -0.5, 0.1875, ((0, 8), (1, 4))),
        "right_ops": normal_values(arg_keys[2], (PAIRS, SECTORS, BLOCK, BLOCK), (BLOCK * PAIRS) ** -0.5, 0.046875, ((0, 8), (1, 4))),
        "targets": set_ends(jax.random.randint(arg_keys[3], (PAIRS, SECTORS), -1, SECTORS), jax.random.fold_in(arg_keys[3], 1), -1, SECTORS - 1).astype(jnp.int32),
        "sector_sizes": set_ends(jax.random.randint(arg_keys[4], (SECTORS,), BLOCK // 4, BLOCK + 1), jax.random.fold_in(arg_keys[4], 1), BLOCK // 4, BLOCK).astype(jnp.int32),
        "pair_ids": jax.random.permutation(arg_keys[5], PAIRS).astype(jnp.int32),
        "pair_coefficients": jnp.clip(jnp.exp(jax.random.uniform(arg_keys[6], (PAIRS,), jnp.float32, math.log(0.25), math.log(2.0))), 0.25, 2.0),
    }


def reference(wave, left_ops, right_ops, targets, sector_sizes, pair_ids, pair_coefficients):
    positions = jnp.arange(BLOCK, dtype=jnp.int32)
    used = (positions[None, :] < sector_sizes[:, None]).astype(wave.dtype)
    masked = wave * used[:, :, None] * used[:, None, :]
    factor = pair_coefficients[pair_ids]
    sector_ids = jnp.arange(SECTORS, dtype=jnp.int32)

    def one_pair(totals, packed):
        left_op, right_op, target, weight = packed
        for source in range(SECTORS):
            left = jnp.dot(left_op[source], masked[source], preferred_element_type=jnp.float32).astype(jnp.bfloat16)
            term = lax.dot_general(left, right_op[source], (((1,), (1,)), ((), ())), preferred_element_type=jnp.float32)
            chosen = (sector_ids == target[source]).astype(jnp.float32)
            totals = totals + chosen[:, None, None] * (weight * term)[None]
        return totals, None

    start_totals = jnp.zeros((SECTORS, BLOCK, BLOCK), jnp.float32)
    totals, _ = lax.scan(one_pair, start_totals, (left_ops, right_ops, targets, factor))
    used_float = used.astype(jnp.float32)
    return totals * used_float[:, :, None] * used_float[:, None, :]
```

```python
import functools

import jax
import jax.numpy as jnp
from jax import lax
from jax.experimental import pallas as pl
from jax.experimental.pallas import tpu as pltpu
from jax.sharding import PartitionSpec as P

MESH = pl.DeviceIdType.MESH
F32 = jnp.float32
LANES = 128
PLANE_DEPTH = 128
ROW_TILE = 512
PIECES = 2
VMEM_LIMIT = 48 * 1024 * 1024


def step_kernel(
    cfg, wave_hbm, targets_ref, sizes_ref, ids_ref, coefs_ref, left_hbm, right_hbm, out_ref,
    wave_ref, wbuf, lbuf, rbuf, acc, left, own, psend, precv, weight_ref, wother,
    xs, xr, ys, yr, zs, zr, fsend, frecv, load_sem, sems_s, sems_r, line_s, line_r, gat_s, gat_r,
):
    Z, X, T, K, rows, block, groups, orders = cfg
    half = block // 2
    pair, sector = lax.axis_index("pair"), lax.axis_index("sector")
    z, x = pair // X, lax.rem(pair, X)
    y, c = sector // 2, lax.rem(sector, 2)

    def dev(zz=None, xx=None, yy=None, cc=None):
        zz, xx = z if zz is None else zz, x if xx is None else xx
        yy, cc = y if yy is None else yy, c if cc is None else cc
        return (zz * X + xx, yy * 2 + cc)

    x_dev, y_dev, c_dev = dev(xx=1 - x), dev(yy=1 - y), dev(cc=1 - c)
    up_dev, dn_dev = dev(zz=z + 1), dev(zz=z - 1)

    def loop(count, f):
        def one(i, carry):
            f(i)
            return carry

        lax.fori_loop(0, count, one, 0)

    has_up, has_dn = z + 1 < Z, z >= 1

    loads = []
    for k in range(K):
        loads.append(pltpu.make_async_copy(left_hbm.at[k], lbuf.at[k], load_sem.at[k]))
        loads.append(pltpu.make_async_copy(right_hbm.at[k], rbuf.at[k], load_sem.at[K + k]))
    barrier = pltpu.get_barrier_semaphore()
    for other in (x_dev, y_dev, c_dev):
        pl.semaphore_signal(barrier, inc=1, device_id=other, device_id_type=MESH)

    wave_load = pltpu.make_async_copy(wave_hbm, wave_ref, load_sem.at[2 * K])
    wave_load.start()

    @pl.when(has_up)
    def _():
        pl.semaphore_signal(barrier, inc=1, device_id=up_dev, device_id_type=MESH)

    @pl.when(has_dn)
    def _():
        pl.semaphore_signal(barrier, inc=1, device_id=dn_dev, device_id_type=MESH)

    for k in range(K):
        factor = coefs_ref[ids_ref[k]]
        for t in range(T):
            chosen = jnp.where(targets_ref[k] == t, factor, 0.0)
            weight_ref[k * T + t] = jnp.full((8, LANES), chosen, F32)
    for g in range(groups):
        for tc in range(2):
            zr[g][tc, z] = jnp.zeros((rows, LANES), jnp.bfloat16)
    for k in range(K):
        loads[2 * k].start()
    size = sizes_ref[sector]
    row_ids = pair * rows + lax.broadcasted_iota(jnp.int32, (rows, LANES), 0)
    lane_ids = lax.broadcasted_iota(jnp.int32, (rows, LANES), 1)

    def used(column):
        return ((row_ids < size) & (lane_ids + column < size)).astype(F32)

    wave_load.wait()
    for at in range(0, block, LANES):
        value = wave_ref[:, at : at + LANES].astype(F32) * used(at)
        wbuf[z, x, :, at : at + LANES] = value.astype(jnp.bfloat16)
    pl.semaphore_wait(barrier, 3 + has_up.astype(jnp.int32) + has_dn.astype(jnp.int32))

    def remote(src, dst, ss, rs, device):
        return pltpu.make_async_remote_copy(
            src_ref=src, dst_ref=dst, send_sem=ss, recv_sem=rs, device_id=device, device_id_type=MESH
        )

    piece = rows // PIECES if rows % (16 * PIECES) == 0 else rows
    pieces = rows // piece

    def block_at(q, xx, p):
        return wbuf.at[q, xx, pl.ds(p * piece, piece)]

    def hop(q, way, p):
        device = (up_dev, dn_dev, x_dev)[way]
        return remote(block_at(q, x, p), block_at(q, x, p), gat_s.at[way, q, p], gat_r.at[q, x, p], device)

    def arrival(q, xx, p):
        return remote(block_at(q, xx, p), block_at(q, xx, p), gat_s.at[2, q, p], gat_r.at[q, xx, p], x_dev)

    def pass_on(q, ways, p):
        if 0 in ways:
            @pl.when(has_up)
            def _():
                hop(q, 0, p).start()

        if 1 in ways:
            @pl.when(has_dn)
            def _():
                hop(q, 1, p).start()

        hop(q, 2, p).start()

    for p in range(pieces):
        pass_on(z, (0, 1), p)
    weights_copy = remote(weight_ref, wother, sems_s.at[0], sems_r.at[0], c_dev)
    weights_copy.start()
    for k in range(K):
        loads[2 * k + 1].start()

    depth = X * rows
    planewise = depth % PLANE_DEPTH == 0
    tile = min(ROW_TILE, block)
    tiles = block // tile

    def multiply(q, first):
        plane = wbuf.at[q]

        def one(i, carry):
            k, at = i // tiles, pl.multiple_of(lax.rem(i, tiles) * tile, tile)
            cols = pl.ds(pl.multiple_of(q * depth, depth), depth)
            product = jnp.dot(
                lbuf[k, pl.ds(at, tile), cols], plane[...].reshape(depth, block), preferred_element_type=F32
            )
            if first:
                acc[k, pl.ds(at, tile), :] = product
            else:
                acc[k, pl.ds(at, tile), :] += product
            return carry

        lax.fori_loop(0, K * tiles, one, 0)

    def take_plane(q, first=False):
        for p in range(pieces):
            arrival(q, 1 - x, p).wait_recv()
        if planewise:
            multiply(q, first)

    for k in range(K):
        loads[2 * k].wait()

    def forward(d, carry):
        lo, hi = z - d, z + d
        for p in range(pieces):
            @pl.when(lo >= 0)
            def _():
                arrival(lo, x, p).wait_recv()
                pass_on(lo, (0,), p)

            @pl.when(hi < Z)
            def _():
                arrival(hi, x, p).wait_recv()
                pass_on(hi, (1,), p)

        @pl.when(d == 1)
        def _():
            take_plane(z, True)

        return carry

    lax.fori_loop(1, Z, forward, 0)

    def take_planes(d, carry):
        @pl.when(z - d >= 0)
        def _():
            take_plane(z - d)

        @pl.when(z + d < Z)
        def _():
            take_plane(z + d)

        return carry

    lax.fori_loop(1, Z, take_planes, 0)

    def finish_left(i, carry):
        k, at = i // tiles, pl.multiple_of(lax.rem(i, tiles) * tile, tile)
        if planewise:
            value = acc[k, pl.ds(at, tile), :]
        else:
            value = jnp.dot(
                lbuf[k, pl.ds(at, tile), :], wbuf[...].reshape(block, block), preferred_element_type=F32
            )
        left[k, pl.ds(at, tile), :] = value.astype(jnp.bfloat16)
        return carry

    lax.fori_loop(0, K * tiles, finish_left, 0)
    for k in range(K):
        loads[2 * k + 1].wait()

    width = 2 * LANES

    def second(part, side, dest):
        def one(i, carry):
            k, at = i // tiles, pl.multiple_of(lax.rem(i, tiles) * tile, tile)
            right_at = pl.multiple_of(side * half + part * width, width)
            term = lax.dot_general(
                left[k, pl.ds(at, tile), :], rbuf[k, pl.ds(right_at, width), :],
                (((1,), (1,)), ((), ())), preferred_element_type=F32,
            )
            for j in range(2):
                dest[2 * part + j, k, pl.ds(at, tile), :] = term[:, j * LANES : (j + 1) * LANES].astype(dest.dtype)
            return carry

        lax.fori_loop(0, K * tiles, one, 0)

    def part_copy(part):
        span = pl.ds(2 * part, 2)
        return remote(psend.at[span], precv.at[span], sems_s.at[1 + part], sems_r.at[1 + part], c_dev)

    base = 1 + groups // 2

    def step_copy(g, number, tc):
        letter = orders[g][number]
        s, r = ((xs, xr), (ys, yr))["xy".index(letter)]
        at = base + 4 * g + 2 * number + tc
        return remote(s[g].at[tc], r[g].at[tc], sems_s.at[at], sems_r.at[at], x_dev if letter == "x" else y_dev)

    def chip_sum(g, ty, tc, zz, xx):
        at = pl.ds(pl.multiple_of((zz * X + xx) * rows, rows), rows)
        t = ty * 2 + tc
        total = None
        for k in range(K):
            mine = own[g, k, at, :] * weight_ref[k * T + t, 0:1, :]
            theirs = precv[g, k, at, :].astype(F32) * wother[k * T + t, 0:1, :]
            total = mine + theirs if total is None else total + mine + theirs
        return total

    def x_first(g, tc):
        def one(zz):
            for ty in range(2):
                xs[g][tc, ty, zz] = chip_sum(g, ty, tc, zz, 1 - x).astype(jnp.bfloat16)

        loop(Z, one)
        step_copy(g, 0, tc).start()

    def y_first(g, tc):
        def one(zz):
            for xx in range(2):
                ys[g][tc, zz, xx] = chip_sum(g, 1 - y, tc, zz, xx).astype(jnp.bfloat16)

        loop(Z, one)
        step_copy(g, 0, tc).start()

    def y_second(g, tc):
        step_copy(g, 0, tc).wait_recv()

        def one(zz):
            value = chip_sum(g, 1 - y, tc, zz, x) + xr[g][tc, 1 - y, zz].astype(F32)
            ys[g][tc, zz] = value.astype(jnp.bfloat16)

        loop(Z, one)
        step_copy(g, 1, tc).start()

    def x_second(g, tc):
        step_copy(g, 0, tc).wait_recv()

        def one(zz):
            value = chip_sum(g, y, tc, zz, 1 - x) + yr[g][tc, zz, 1 - x].astype(F32)
            xs[g][tc, zz] = value.astype(jnp.bfloat16)

        loop(Z, one)
        step_copy(g, 1, tc).start()

    def plane_sum(g, tc, zz):
        value = chip_sum(g, y, tc, zz, x)
        if orders[g][0] == "x":
            return value + xr[g][tc, y, zz].astype(F32) + yr[g][tc, zz].astype(F32)
        return value + yr[g][tc, zz, x].astype(F32) + xr[g][tc, zz].astype(F32)

    def line_copy(g, tc, zz):
        return remote(
            zs[g].at[tc, zz], zr[g].at[tc, z], line_s.at[g, tc, zz], line_r.at[g, tc, z], dev(zz=zz)
        )

    def line_arrival(g, tc, zz):
        return remote(
            zs[g].at[tc, zz], zr[g].at[tc, zz], line_s.at[g, tc, zz], line_r.at[g, tc, zz], dev(zz=zz)
        )

    def line(g, tc):
        step_copy(g, 1, tc).wait_recv()

        def one(j):
            zz = lax.rem(z + 1 + j, Z)
            zs[g][tc, zz] = plane_sum(g, tc, zz).astype(jnp.bfloat16)
            line_copy(g, tc, zz).start()

        loop(Z - 1, one)

    def total(g, tc):
        value = plane_sum(g, tc, z)
        if Z <= 8:
            for zz in range(Z):
                value = value + zr[g][tc, zz].astype(F32)
            return value
        return lax.fori_loop(0, Z, lambda zz, v: v + zr[g][tc, zz].astype(F32), value)

    def final_copy(g):
        at = base + 4 * groups + g
        return remote(fsend.at[g], frecv.at[g], sems_s.at[at], sems_r.at[at], c_dev)

    def finish(g):
        def wait(j):
            for tc in range(2):
                line_arrival(g, tc, lax.rem(z + 1 + j, Z)).wait_recv()

        loop(Z - 1, wait)
        fsend[g] = total(g, 1 - c)
        final_copy(g).start()
        at = pl.multiple_of(c * half + g * LANES, LANES)
        out_ref[:, pl.ds(at, LANES)] = total(g, c) * used(at)

    def first(i):
        x_first(2 * (i // 2), i % 2)
        y_first(2 * (i // 2) + 1, i % 2)

    def next_step(i):
        y_second(2 * (i // 2), i % 2)
        x_second(2 * (i // 2) + 1, i % 2)

    def lines(i):
        line(2 * (i // 2), i % 2)
        line(2 * (i // 2) + 1, i % 2)

    parts = groups // 2
    rounds = groups
    second(0, 1 - c, psend)
    part_copy(0).start()
    second(0, c, own)
    weights_copy.wait_recv()
    for i in range(rounds):
        part = i // 2
        if i % 2 == 0:
            if part + 1 < parts:
                second(part + 1, 1 - c, psend)
                part_copy(part + 1).start()
            part_copy(part).wait_recv()
        first(i)
        if i % 2 == 1 and part + 1 < parts:
            second(part + 1, c, own)
        if i >= 1:
            next_step(i - 1)
        if i >= 2:
            lines(i - 2)
    next_step(rounds - 1)
    lines(rounds - 2)
    for g in range(groups - 2):
        finish(g)
    lines(rounds - 1)
    for g in range(groups - 2, groups):
        finish(g)
    for g in range(groups):
        final_copy(g).wait_recv()
        at = pl.multiple_of((1 - c) * half + g * LANES, LANES)
        out_ref[:, pl.ds(at, LANES)] = frecv[g] * used(at)

    def drain(q):
        for p in range(pieces):
            @pl.when(jnp.logical_and(has_up, q <= z))
            def _():
                hop(q, 0, p).wait_send()

            @pl.when(jnp.logical_and(has_dn, q >= z))
            def _():
                hop(q, 1, p).wait_send()

            hop(q, 2, p).wait_send()

    loop(Z, drain)
    weights_copy.wait_send()
    for part in range(parts):
        part_copy(part).wait_send()
    for g in range(groups):
        final_copy(g).wait_send()
        for tc in range(2):
            step_copy(g, 0, tc).wait_send()
            step_copy(g, 1, tc).wait_send()

            def drain_line(j, g=g, tc=tc):
                line_copy(g, tc, lax.rem(z + 1 + j, Z)).wait_send()

            loop(Z - 1, drain_line)


def kernel_entry(cfg, *refs):
    groups = cfg[6]
    ins, scratch = refs[:8], list(refs[8:])
    plain = scratch[:11]
    per_group = [scratch[11 + n * groups : 11 + (n + 1) * groups] for n in range(6)]
    step_kernel(cfg, *ins, *plain, *per_group, *scratch[11 + 6 * groups :])


def body(wave, left_ops, right_ops, targets, sector_sizes, pair_ids, pair_coefficients):
    block = wave.shape[2]
    rows = wave.shape[1]
    K = left_ops.shape[0]
    T = sector_sizes.shape[0]
    pairs = lax.axis_size("pair")
    X = 2
    Z = pairs // X
    half = block // 2
    groups = half // LANES
    orders = tuple(("xyz", "yxz")[g % 2] for g in range(groups))
    bf = jnp.bfloat16
    xs, xr, ys, yr, zs, zr = [], [], [], [], [], []
    for order in orders:
        tail = (rows, LANES)
        x_shape, y_shape = {"x": ((2, 2, Z), (2, Z)), "y": ((2, Z), (2, Z, X))}[order[0]]
        for where, shape in ((xs, x_shape), (xr, x_shape), (ys, y_shape), (yr, y_shape), (zs, (2, Z)), (zr, (2, Z))):
            where.append(pltpu.VMEM(shape + tail, bf))
    count = 1 + groups // 2 + 5 * groups
    dma = pltpu.SemaphoreType.DMA
    cfg = (Z, X, T, K, rows, block, groups, orders)
    planewise = (X * rows) % PLANE_DEPTH == 0
    vmem, hbm = pl.BlockSpec(memory_space=pltpu.VMEM), pl.BlockSpec(memory_space=pltpu.HBM)
    smem = pl.BlockSpec(memory_space=pltpu.SMEM)
    out = pl.pallas_call(
        functools.partial(kernel_entry, cfg),
        out_shape=jax.ShapeDtypeStruct((rows, block), F32),
        in_specs=[hbm, smem, smem, smem, smem, hbm, hbm],
        out_specs=vmem,
        scratch_shapes=[
            pltpu.VMEM((rows, block), bf),
            pltpu.VMEM((Z, X, rows, block), bf),
            pltpu.VMEM((K, block, block), bf),
            pltpu.VMEM((K, block, block), bf),
            pltpu.VMEM((K, block, block) if planewise else (8, LANES), F32),
            pltpu.VMEM((K, block, block), bf),
            pltpu.VMEM((groups, K, block, LANES), F32),
            pltpu.VMEM((groups, K, block, LANES), F32),
            pltpu.VMEM((groups, K, block, LANES), F32),
            pltpu.VMEM((K * T, 8, LANES), F32),
            pltpu.VMEM((K * T, 8, LANES), F32),
            *xs, *xr, *ys, *yr, *zs, *zr,
            pltpu.VMEM((groups, rows, LANES), F32),
            pltpu.VMEM((groups, rows, LANES), F32),
            dma((2 * K + 1,)), dma((count,)), dma((count,)),
            dma((groups, 2, Z)), dma((groups, 2, Z)), dma((3, Z, PIECES)), dma((Z, X, PIECES)),
        ],
        compiler_params=pltpu.CompilerParams(
            collective_id=0, has_side_effects=True, vmem_limit_bytes=VMEM_LIMIT
        ),
        name="sigma_step",
    )(wave[0], targets.reshape(-1), sector_sizes, pair_ids, pair_coefficients, left_ops[:, 0], right_ops[:, 0])
    return out[None]


def solution(mesh):
    placed = (
        P("sector", "pair", None),
        P("pair", "sector", None, None),
        P("pair", "sector", None, None),
        P("pair", "sector"),
        P(),
        P("pair"),
        P(),
    )
    return jax.shard_map(
        body, mesh=mesh, in_specs=placed, out_specs=P("sector", "pair", None), check_vma=False
    )
```

```python
import functools

import jax
import jax.numpy as jnp
from jax import lax
from jax.experimental import pallas as pl
from jax.experimental.pallas import tpu as pltpu
from jax.sharding import PartitionSpec as P

MESH = pl.DeviceIdType.MESH
F32 = jnp.float32
BF16 = jnp.bfloat16
LANES = 128
PLANE_DEPTH = 128
ROW_TILE = 512
PIECES = 2
VMEM_LIMIT = 48 * 1024 * 1024
KINDS = ("xs", "xr", "ys", "yr", "zs", "zr")


def plan(groups, split):
    if split == 2:
        pairs = [[(g, tc, h) for h in range(2)] for g in range(groups) for tc in range(2)]
    else:
        pairs = [[(g, tc, 0) for tc in range(2)] for g in range(groups)]
    orders = [("zxy", "zyx") if n == 1 else ("xyz", "yxz") for n in range(len(pairs))]
    return [[unit + (order,) for unit, order in zip(pair, way)] for pair, way in zip(pairs, orders)]


def step_kernel(
    cfg, wave_hbm, targets_ref, sizes_ref, ids_ref, coefs_ref, left_hbm, right_hbm, out_ref,
    wave_ref, wbuf, lbuf, rbuf, acc, left, own, psend, precv, weight_ref, wother, fsend, frecv,
    load_sem, sems_s, sems_r, line_s, line_r, gat_s, gat_r, relay_s, bufs,
):
    Z, X, T, K, rows, block, groups, split, pairs = cfg
    units = [unit for pair in pairs for unit in pair]
    half = block // 2
    pair, sector = lax.axis_index("pair"), lax.axis_index("sector")
    z, x = pair // X, lax.rem(pair, X)
    y, c = sector // 2, lax.rem(sector, 2)

    def dev(zz=None, xx=None, yy=None, cc=None):
        zz, xx = z if zz is None else zz, x if xx is None else xx
        yy, cc = y if yy is None else yy, c if cc is None else cc
        return (zz * X + xx, yy * 2 + cc)

    x_dev, y_dev, c_dev = dev(xx=1 - x), dev(yy=1 - y), dev(cc=1 - c)
    up_dev, dn_dev = dev(zz=z + 1), dev(zz=z - 1)

    def loop(count, f):
        def one(i, carry):
            f(i)
            return carry

        lax.fori_loop(0, count, one, 0)

    has_up, has_dn = z + 1 < Z, z >= 1

    left_loads = [pltpu.make_async_copy(left_hbm.at[k], lbuf.at[k], load_sem.at[k]) for k in range(K)]
    right_loads = []
    for k in range(K):
        for g in range(groups):
            for j in range(2):
                at = pl.multiple_of((1 - c if j == 0 else c) * half + g * LANES, LANES)
                right_loads.append(
                    pltpu.make_async_copy(
                        right_hbm.at[k, pl.ds(at, LANES)], rbuf.at[k, g, j],
                        load_sem.at[K + 1 + (k * groups + g) * 2 + j],
                    )
                )

    barrier = pltpu.get_barrier_semaphore()
    for other in (x_dev, y_dev, c_dev):
        pl.semaphore_signal(barrier, inc=1, device_id=other, device_id_type=MESH)

    wave_load = pltpu.make_async_copy(wave_hbm, wave_ref, load_sem.at[K])
    wave_load.start()

    @pl.when(has_up)
    def _():
        pl.semaphore_signal(barrier, inc=1, device_id=up_dev, device_id_type=MESH)

    @pl.when(has_dn)
    def _():
        pl.semaphore_signal(barrier, inc=1, device_id=dn_dev, device_id_type=MESH)

    for k in range(K):
        factor = coefs_ref[ids_ref[k]]
        for t in range(T):
            chosen = jnp.where(targets_ref[k] == t, factor, 0.0)
            weight_ref[k * T + t] = jnp.full((8, LANES), chosen, F32)
    for n in range(len(units)):
        mine = bufs["zr"][n].at[z]
        mine[...] = jnp.zeros(mine.shape, BF16)
    for copy in left_loads:
        copy.start()
    size = sizes_ref[sector]

    def used(column, start=0, count=rows):
        row_ids = pair * rows + start + lax.broadcasted_iota(jnp.int32, (count, LANES), 0)
        lane_ids = column + lax.broadcasted_iota(jnp.int32, (count, LANES), 1)
        return ((row_ids < size) & (lane_ids < size)).astype(F32)

    wave_load.wait()
    for at in range(0, block, LANES):
        value = wave_ref[:, at : at + LANES].astype(F32) * used(at)
        wbuf[z, x, :, at : at + LANES] = value.astype(jnp.bfloat16)
    pl.semaphore_wait(barrier, 3 + has_up.astype(jnp.int32) + has_dn.astype(jnp.int32))

    def remote(src, dst, ss, rs, device):
        return pltpu.make_async_remote_copy(
            src_ref=src, dst_ref=dst, send_sem=ss, recv_sem=rs, device_id=device, device_id_type=MESH
        )

    piece = rows // PIECES if rows % (16 * PIECES) == 0 else rows
    pieces = rows // piece

    def block_at(q, xx, p):
        return wbuf.at[q, xx, pl.ds(p * piece, piece)]

    def hop(q, way, p):
        device = (up_dev, dn_dev, x_dev)[way]
        return remote(block_at(q, x, p), block_at(q, x, p), gat_s.at[way, q, p], gat_r.at[q, x, p], device)

    def arrival(q, xx, p):
        return remote(block_at(q, xx, p), block_at(q, xx, p), gat_s.at[2, q, p], gat_r.at[q, xx, p], x_dev)

    relayed = Z >= 3 and pieces >= 2
    last = pieces - 1

    def skips_x(q, p):
        if not relayed or p != last:
            return jnp.bool_(False)
        return ((z == 0) & (q == 1)) | ((z == Z - 1) & (q == Z - 2))

    def relay(way):
        device = (up_dev, dn_dev)[way]
        block_there = block_at(z, 1 - x, last)
        return remote(block_there, block_there, relay_s.at[way], gat_r.at[z, 1 - x, last], device)

    def relays(f):
        if relayed:
            @pl.when(z == Z - 2)
            def _():
                f(relay(0))

            @pl.when(z == 1)
            def _():
                f(relay(1))

    def pass_on(q, ways, p):
        if 0 in ways:
            @pl.when(has_up)
            def _():
                hop(q, 0, p).start()

        if 1 in ways:
            @pl.when(has_dn)
            def _():
                hop(q, 1, p).start()

        @pl.when(jnp.logical_not(skips_x(q, p)))
        def _():
            hop(q, 2, p).start()

    for p in range(pieces):
        pass_on(z, (0, 1), p)
    weights_copy = remote(weight_ref, wother, sems_s.at[0], sems_r.at[0], c_dev)
    weights_copy.start()
    for copy in right_loads:
        copy.start()

    depth = X * rows
    planewise = depth % PLANE_DEPTH == 0
    tile = min(ROW_TILE, block)
    tiles = block // tile

    def multiply(q, stage):
        plane = wbuf.at[q]

        def one(i, carry):
            k, at = i // tiles, pl.multiple_of(lax.rem(i, tiles) * tile, tile)
            cols = pl.ds(pl.multiple_of(q * depth, depth), depth)
            product = jnp.dot(
                lbuf[k, pl.ds(at, tile), cols], plane[...].reshape(depth, block), preferred_element_type=F32
            )
            if stage == "only":
                left[k, pl.ds(at, tile), :] = product.astype(BF16)
            elif stage == "first":
                acc[k, pl.ds(at, tile), :] = product
            elif stage == "middle":
                acc[k, pl.ds(at, tile), :] += product
            else:
                left[k, pl.ds(at, tile), :] = (acc[k, pl.ds(at, tile), :] + product).astype(BF16)
            return carry

        lax.fori_loop(0, K * tiles, one, 0)

    def take_plane(q, stage):
        for p in range(pieces):
            arrival(q, 1 - x, p).wait_recv()
        if stage in ("first", "only"):
            relays(lambda copy: copy.start())
        if planewise:
            multiply(q, stage)

    for copy in left_loads:
        copy.wait()

    def forward(d, carry):
        lo, hi = z - d, z + d
        for p in range(pieces):
            @pl.when(lo >= 0)
            def _():
                arrival(lo, x, p).wait_recv()
                pass_on(lo, (0,), p)

            @pl.when(hi < Z)
            def _():
                arrival(hi, x, p).wait_recv()
                pass_on(hi, (1,), p)

        @pl.when(d == 1)
        def _():
            take_plane(z, "first")

        return carry

    if Z == 1:
        take_plane(z, "only")
    lax.fori_loop(1, Z, forward, 0)
    near = jnp.minimum(z, Z - 1 - z)

    def plane_by_distance(i):
        d = (i + 1) // 2
        both = jnp.where(lax.rem(i, 2) == 1, z - d, z + d)
        return jnp.where(i <= 2 * near, both, jnp.where(z > near, z - (i - near), z + (i - near)))

    def take_planes(i, carry):
        take_plane(plane_by_distance(i), "middle")
        return carry

    lax.fori_loop(1, Z - 1, take_planes, 0)
    if Z > 1:
        take_plane(plane_by_distance(jnp.int32(Z - 1)), "last")

    def whole_left(i, carry):
        k, at = i // tiles, pl.multiple_of(lax.rem(i, tiles) * tile, tile)
        value = jnp.dot(
            lbuf[k, pl.ds(at, tile), :], wbuf[...].reshape(block, block), preferred_element_type=F32
        )
        left[k, pl.ds(at, tile), :] = value.astype(BF16)
        return carry

    if not planewise:
        lax.fori_loop(0, K * tiles, whole_left, 0)
    for copy in right_loads:
        copy.wait()

    def core_copy(g, k):
        at = 1 + g * K + k
        return remote(psend.at[g, k], precv.at[g, k], sems_s.at[at], sems_r.at[at], c_dev)

    def second(g, k):
        def one(i, carry):
            at = pl.multiple_of(i * tile, tile)
            term = lax.dot_general(
                left[k, pl.ds(at, tile), :], rbuf[k, g].reshape(2 * LANES, block),
                (((1,), (1,)), ((), ())), preferred_element_type=F32,
            )
            psend[g, k, pl.ds(at, tile), :] = term[:, :LANES].astype(BF16)
            own[g, k, pl.ds(at, tile), :] = term[:, LANES:]
            return carry

        lax.fori_loop(0, tiles, one, 0)
        core_copy(g, k).start()

    part = rows // split

    def chip_sum(n, ty, zz, xx):
        g, tc, h, _ = units[n]
        at = pl.ds(pl.multiple_of((zz * X + xx) * rows + h * part, part), part)
        t = ty * 2 + tc
        total = None
        for k in range(K):
            mine = own[g, k, at, :] * weight_ref[k * T + t, 0:1, :]
            theirs = precv[g, k, at, :].astype(F32) * wother[k * T + t, 0:1, :]
            total = mine + theirs if total is None else total + mine + theirs
        return total

    base = 1 + K * groups
    xs, xr, ys, yr, zs, zr = (bufs[kind] for kind in KINDS)

    def step_copy(n, letter):
        s, r = (xs, xr) if letter == "x" else (ys, yr)
        at = base + 2 * n + "xy".index(letter)
        return remote(s[n], r[n], sems_s.at[at], sems_r.at[at], x_dev if letter == "x" else y_dev)

    def line_copy(n, zz):
        return remote(zs[n].at[zz], zr[n].at[z], line_s.at[n, zz], line_r.at[n, z], dev(zz=zz))

    def line_arrival(n, zz):
        return remote(zs[n].at[zz], zr[n].at[zz], line_s.at[n, zz], line_r.at[n, zz], dev(zz=zz))

    def others(f):
        loop(Z - 1, lambda j: f(lax.rem(z + 1 + j, Z)))

    def send(n):
        order = units[n][3]
        if order == "xyz":
            def one(zz):
                for ty in range(2):
                    xs[n][ty, zz] = chip_sum(n, ty, zz, 1 - x).astype(BF16)

            loop(Z, one)
            step_copy(n, "x").start()
        elif order == "yxz":
            def one(zz):
                for xx in range(X):
                    ys[n][zz, xx] = chip_sum(n, 1 - y, zz, xx).astype(BF16)

            loop(Z, one)
            step_copy(n, "y").start()
        else:
            def one(zz):
                for ty in range(2):
                    for xx in range(X):
                        zs[n][zz, ty, xx] = chip_sum(n, ty, zz, xx).astype(BF16)
                line_copy(n, zz).start()

            others(one)

    def line_sum(n, value, pick):
        if Z <= 8:
            for zz in range(Z):
                value = value + pick(zr[n].at[zz])[...].astype(F32)
            return value
        return lax.fori_loop(0, Z, lambda zz, v: v + pick(zr[n].at[zz])[...].astype(F32), value)

    def summed(n, ty, xx):
        return line_sum(n, chip_sum(n, ty, z, xx), lambda ref: ref.at[ty, xx])

    def send_again(n):
        order = units[n][3]
        if order == "xyz":
            step_copy(n, "x").wait_recv()

            def one(zz):
                value = chip_sum(n, 1 - y, zz, x) + xr[n][1 - y, zz].astype(F32)
                ys[n][zz] = value.astype(BF16)

            loop(Z, one)
            step_copy(n, "y").start()
        elif order == "yxz":
            step_copy(n, "y").wait_recv()

            def one(zz):
                value = chip_sum(n, y, zz, 1 - x) + yr[n][zz, 1 - x].astype(F32)
                xs[n][zz] = value.astype(BF16)

            loop(Z, one)
            step_copy(n, "x").start()
        else:
            others(lambda zz: line_arrival(n, zz).wait_recv())
            for j in range(2):
                if order == "zxy":
                    xs[n][j] = summed(n, j, 1 - x).astype(BF16)
                else:
                    ys[n][j] = summed(n, 1 - y, j).astype(BF16)
            step_copy(n, order[1]).start()

    def plane_sum(n, zz):
        value = chip_sum(n, y, zz, x)
        if units[n][3] == "xyz":
            return value + xr[n][y, zz].astype(F32) + yr[n][zz].astype(F32)
        return value + yr[n][zz, x].astype(F32) + xr[n][zz].astype(F32)

    def send_last(n):
        order = units[n][3]
        if order[2] == "z":
            step_copy(n, order[1]).wait_recv()

            def one(zz):
                zs[n][zz] = plane_sum(n, zz).astype(BF16)
                line_copy(n, zz).start()

            others(one)
        elif order == "zxy":
            step_copy(n, "x").wait_recv()
            ys[n][...] = (summed(n, 1 - y, x) + xr[n][1 - y].astype(F32)).astype(BF16)
            step_copy(n, "y").start()
        else:
            step_copy(n, "y").wait_recv()
            xs[n][...] = (summed(n, y, 1 - x) + yr[n][1 - x].astype(F32)).astype(BF16)
            step_copy(n, "x").start()

    def total(n):
        order = units[n][3]
        if order[2] == "z":
            others(lambda zz: line_arrival(n, zz).wait_recv())
            return line_sum(n, plane_sum(n, z), lambda ref: ref)
        step_copy(n, order[2]).wait_recv()
        value = summed(n, y, x)
        if order == "zxy":
            return value + xr[n][y].astype(F32) + yr[n][...].astype(F32)
        return value + yr[n][x].astype(F32) + xr[n][...].astype(F32)

    def final_copy(g):
        at = base + 2 * len(units) + g
        return remote(fsend.at[g], frecv.at[g], sems_s.at[at], sems_r.at[at], c_dev)

    def finish(g):
        at = pl.multiple_of(c * half + g * LANES, LANES)
        for h in range(split):
            span = pl.ds(h * part, part)
            one, two = (total(units.index((g, tc, h, order_of[g, tc, h]))) for tc in range(2))
            out_ref[span, pl.ds(at, LANES)] = jnp.where(c == 0, one, two) * used(at, h * part, part)
            fsend[g, span, :] = jnp.where(c == 0, two, one)
        final_copy(g).start()

    order_of = {unit[:3]: unit[3] for unit in units}
    numbers = [[units.index(unit) for unit in pair] for pair in pairs]
    plain = [pair for i, pair in enumerate(numbers) if i != 1]
    turned = numbers[1]

    def group_of(j):
        return units[plain[j][0]][0]

    def each(f, pair):
        for n in pair:
            f(n)

    ready = set()

    def receive(g):
        if g not in ready:
            ready.add(g)
            for k in range(K):
                core_copy(g, k).wait_recv()

    queue = [(g, k) for g in range(groups) for k in range(K)]

    def compute(count):
        for _ in range(min(count, len(queue))):
            second(*queue.pop(0))

    def compute_to(g):
        while queue and queue[0][0] <= g:
            compute(1)

    steps = len(plain)
    compute(K + 1)
    weights_copy.wait_recv()
    receive(0)
    each(send, plain[0])
    each(send, turned)
    compute_to(group_of(1))
    receive(group_of(1))
    each(send, plain[1])
    compute(K)
    for j in range(steps):
        each(send_again, plain[j])
        if j + 2 < steps:
            compute_to(group_of(j + 2))
            receive(group_of(j + 2))
            each(send, plain[j + 2])
            compute(1)
        if j == steps - 1:
            each(send_again, turned)
        if j >= 1:
            each(send_last, plain[j - 1])
    each(send_last, plain[steps - 1])
    each(send_last, turned)
    for g in (*range(1, groups - 1), 0, groups - 1):
        finish(g)
    for g in range(groups):
        final_copy(g).wait_recv()
        at = pl.multiple_of((1 - c) * half + g * LANES, LANES)
        out_ref[:, pl.ds(at, LANES)] = frecv[g] * used(at)

    def drain(q):
        for p in range(pieces):
            @pl.when(jnp.logical_and(has_up, q <= z))
            def _():
                hop(q, 0, p).wait_send()

            @pl.when(jnp.logical_and(has_dn, q >= z))
            def _():
                hop(q, 1, p).wait_send()

            @pl.when(jnp.logical_not(skips_x(q, p)))
            def _():
                hop(q, 2, p).wait_send()

    loop(Z, drain)
    relays(lambda copy: copy.wait_send())
    weights_copy.wait_send()
    for g in range(groups):
        final_copy(g).wait_send()
        for k in range(K):
            core_copy(g, k).wait_send()
    for n in range(len(units)):
        step_copy(n, "x").wait_send()
        step_copy(n, "y").wait_send()
        others(lambda zz, n=n: line_copy(n, zz).wait_send())


def kernel_entry(cfg, *refs):
    count = len([unit for pair in cfg[8] for unit in pair])
    plain, rest = refs[:21], refs[21:]
    bufs = {kind: rest[i * count : (i + 1) * count] for i, kind in enumerate(KINDS)}
    step_kernel(cfg, *plain, *rest[len(KINDS) * count :], bufs)


def unit_shapes(order, Z, X, tail):
    lead = {
        "xyz": ((2, Z), (Z,), (Z,)),
        "yxz": ((Z,), (Z, X), (Z,)),
        "zxy": ((2,), (), (Z, 2, X)),
        "zyx": ((), (X,), (Z, 2, X)),
    }[order]
    return [pltpu.VMEM(shape + tail, BF16) for shape in lead]


def body(wave, left_ops, right_ops, targets, sector_sizes, pair_ids, pair_coefficients):
    block = wave.shape[2]
    rows = wave.shape[1]
    K = left_ops.shape[0]
    T = sector_sizes.shape[0]
    pairs = lax.axis_size("pair")
    X = 2
    Z = pairs // X
    half = block // 2
    groups = half // LANES
    split = 2 if rows % 32 == 0 else 1
    unit_pairs = plan(groups, split)
    units = [unit for pair in unit_pairs for unit in pair]
    shapes = [unit_shapes(unit[3], Z, X, (rows // split, LANES)) for unit in units]
    unit_bufs = [shape[axis] for axis in range(3) for _ in range(2) for shape in shapes]
    count = 1 + K * groups + 2 * len(units) + groups
    dma = pltpu.SemaphoreType.DMA
    cfg = (Z, X, T, K, rows, block, groups, split, unit_pairs)
    planewise = (X * rows) % PLANE_DEPTH == 0
    vmem, hbm = pl.BlockSpec(memory_space=pltpu.VMEM), pl.BlockSpec(memory_space=pltpu.HBM)
    smem = pl.BlockSpec(memory_space=pltpu.SMEM)
    operands = (
        wave[0], targets.reshape(-1), sector_sizes, pair_ids, pair_coefficients, left_ops[:, 0], right_ops[:, 0]
    )
    out = pl.pallas_call(
        functools.partial(kernel_entry, cfg),
        out_shape=jax.ShapeDtypeStruct((rows, block), F32),
        in_specs=[hbm, smem, smem, smem, smem, hbm, hbm],
        out_specs=vmem,
        scratch_shapes=[
            pltpu.VMEM((rows, block), BF16),
            pltpu.VMEM((Z, X, rows, block), BF16),
            pltpu.VMEM((K, block, block), BF16),
            pltpu.VMEM((K, groups, 2, LANES, block), BF16),
            pltpu.VMEM((K, block, block) if planewise else (8, LANES), F32),
            pltpu.VMEM((K, block, block), BF16),
            pltpu.VMEM((groups, K, block, LANES), F32),
            pltpu.VMEM((groups, K, block, LANES), BF16),
            pltpu.VMEM((groups, K, block, LANES), BF16),
            pltpu.VMEM((K * T, 8, LANES), F32),
            pltpu.VMEM((K * T, 8, LANES), F32),
            pltpu.VMEM((groups, rows, LANES), F32),
            pltpu.VMEM((groups, rows, LANES), F32),
            *unit_bufs,
            dma((K + 1 + 2 * K * groups,)), dma((count,)), dma((count,)),
            dma((len(units), Z)), dma((len(units), Z)), dma((3, Z, PIECES)), dma((Z, X, PIECES)), dma((2,)),
        ],
        compiler_params=pltpu.CompilerParams(
            collective_id=0, has_side_effects=True, vmem_limit_bytes=VMEM_LIMIT
        ),
        name="sigma_step",
    )(*(pltpu.with_memory_space_constraint(a, pltpu.HBM) for a in operands))
    return out[None]


def solution(mesh):
    placed = (
        P("sector", "pair", None),
        P("pair", "sector", None, None),
        P("pair", "sector", None, None),
        P("pair", "sector"),
        P(),
        P("pair"),
        P(),
    )
    return jax.shard_map(
        body, mesh=mesh, in_specs=placed, out_specs=P("sector", "pair", None), check_vma=False
    )
```

```python
import functools

import jax
import jax.numpy as jnp
from jax import lax
from jax.experimental import pallas as pl
from jax.experimental.pallas import tpu as pltpu
from jax.sharding import PartitionSpec as P

MESH = pl.DeviceIdType.MESH
F32 = jnp.float32
BF16 = jnp.bfloat16
LANES = 128
PLANE_DEPTH = 128
ROW_TILE = 512
PIECES = 2
VMEM_LIMIT = 48 * 1024 * 1024


class Unit:
    def __init__(self, group, core, start, count, order):
        self.group, self.core, self.start, self.count, self.order = group, core, start, count, order


def plan(groups, rows):
    pairs = []
    for g in range(groups):
        parts = 1 if rows % 32 else 4 if g == groups - 1 and rows % 64 == 0 else 2
        count = rows // parts
        if parts == 1:
            found = [[(g, tc, 0, rows) for tc in range(2)]]
        else:
            found = [
                [(g, tc, (i + h) * count, count) for h in range(2)] for tc in range(2) for i in range(0, parts, 2)
            ]
        pairs += found
    orders = [("zxy", "zyx") if n == 1 else ("xyz", "yxz") for n in range(len(pairs))]
    return [[Unit(*part, order) for part, order in zip(pair, way)] for pair, way in zip(pairs, orders)]


def unit_sizes(unit, Z, X):
    return {
        "xyz": (2 * Z, Z, Z),
        "yxz": (Z, Z * X, Z),
        "zxy": (2, 1, Z * 2 * X),
        "zyx": (1, X, Z * 2 * X),
    }[unit.order]


def step_kernel(
    cfg, wave_hbm, targets_hbm, sizes_hbm, ids_hbm, coefs_hbm, left_hbm, right_hbm, out_ref,
    targets_ref, sizes_ref, ids_ref, coefs_ref,
    wave_ref, wbuf, lbuf, rbuf, acc, left, own, psend, precv, weight_ref, wother, fsend, frecv,
    xs, xr, ys, yr, zs, zr, load_sem, send_sem, recv_sem, pair_sem, gat_s, gat_r, relay_s,
):
    Z, X, T, K, rows, block, groups, pairs = cfg
    units = [unit for pair in pairs for unit in pair]
    offsets, ends = [], [0, 0, 0]
    for unit in units:
        offsets.append(tuple(ends))
        ends = [end + size * unit.count for end, size in zip(ends, unit_sizes(unit, Z, X))]
    half = block // 2
    pair, sector = lax.axis_index("pair"), lax.axis_index("sector")
    z, x = pair // X, lax.rem(pair, X)
    y, c = sector // 2, lax.rem(sector, 2)

    def dev(zz=None, xx=None, yy=None, cc=None):
        zz, xx = z if zz is None else zz, x if xx is None else xx
        yy, cc = y if yy is None else yy, c if cc is None else cc
        return (zz * X + xx, yy * 2 + cc)

    x_dev, y_dev, c_dev = dev(xx=1 - x), dev(yy=1 - y), dev(cc=1 - c)
    up_dev, dn_dev = dev(zz=z + 1), dev(zz=z - 1)

    def loop(count, f):
        def one(i, carry):
            f(i)
            return carry

        lax.fori_loop(0, count, one, 0)

    has_up, has_dn = z + 1 < Z, z >= 1

    left_loads = [pltpu.make_async_copy(left_hbm.at[k], lbuf.at[k], load_sem.at[0]) for k in range(K)]
    right_loads = []
    for k in range(K):
        for g in range(groups):
            for j in range(2):
                at = pl.multiple_of((1 - c if j == 0 else c) * half + g * LANES, LANES)
                right_loads.append(
                    pltpu.make_async_copy(
                        right_hbm.at[k, pl.ds(at, LANES)], rbuf.at[k, g, j],
                        load_sem.at[1],
                    )
                )

    barrier = pltpu.get_barrier_semaphore()
    for other in (x_dev, y_dev, c_dev):
        pl.semaphore_signal(barrier, inc=1, device_id=other, device_id_type=MESH)

    wave_load = pltpu.make_async_copy(wave_hbm, wave_ref, load_sem.at[2])
    wave_load.start()
    small_loads = [
        pltpu.make_async_copy(src, dst, load_sem.at[3 + i])
        for i, (src, dst) in enumerate(
            ((targets_hbm, targets_ref), (sizes_hbm, sizes_ref), (ids_hbm, ids_ref), (coefs_hbm, coefs_ref))
        )
    ]
    for copy in small_loads:
        copy.start()

    @pl.when(has_up)
    def _():
        pl.semaphore_signal(barrier, inc=1, device_id=up_dev, device_id_type=MESH)

    @pl.when(has_dn)
    def _():
        pl.semaphore_signal(barrier, inc=1, device_id=dn_dev, device_id_type=MESH)

    def rows_of(n, axis, index):
        count = units[n].count
        return pl.ds(pl.multiple_of(offsets[n][axis] + index * count, count), count)

    def z_index(n, zz, ty=0, xx=0):
        return zz if units[n].order[2] == "z" else (zz * 2 + ty) * X + xx

    for n, unit in enumerate(units):
        size = unit_sizes(unit, Z, X)[2] // Z * unit.count
        zr[pl.ds(pl.multiple_of(offsets[n][2] + z * size, unit.count), size), :] = jnp.zeros((size, LANES), BF16)
    for copy in left_loads:
        copy.start()
    for copy in small_loads:
        copy.wait()
    for k in range(K):
        factor = coefs_ref[ids_ref[k]]
        for t in range(T):
            chosen = jnp.where(targets_ref[k] == t, factor, 0.0)
            weight_ref[k * T + t] = jnp.full((8, LANES), chosen, F32)
    size = sizes_ref[sector]

    def used(column, start=0, count=rows):
        row_ids = pair * rows + start + lax.broadcasted_iota(jnp.int32, (count, LANES), 0)
        lane_ids = column + lax.broadcasted_iota(jnp.int32, (count, LANES), 1)
        return ((row_ids < size) & (lane_ids < size)).astype(F32)

    wave_load.wait()
    for at in range(0, block, LANES):
        value = wave_ref[:, at : at + LANES].astype(F32) * used(at)
        wbuf[z, x, :, at : at + LANES] = value.astype(jnp.bfloat16)
    pl.semaphore_wait(barrier, 3 + has_up.astype(jnp.int32) + has_dn.astype(jnp.int32))

    def remote(src, dst, ss, rs, device):
        return pltpu.make_async_remote_copy(
            src_ref=src, dst_ref=dst, send_sem=ss, recv_sem=rs, device_id=device, device_id_type=MESH
        )

    piece = rows // PIECES if rows % (16 * PIECES) == 0 else rows
    pieces = rows // piece

    def block_at(q, xx, p):
        return wbuf.at[q, xx, pl.ds(p * piece, piece)]

    def hop(q, way, p):
        device = (up_dev, dn_dev, x_dev)[way]
        return remote(block_at(q, x, p), block_at(q, x, p), gat_s.at[way], gat_r.at[q, x, p], device)

    def arrival(q, xx, p):
        return remote(block_at(q, xx, p), block_at(q, xx, p), gat_s.at[2], gat_r.at[q, xx, p], x_dev)

    relayed = Z >= 3 and pieces >= 2
    last = pieces - 1

    def skips_x(q, p):
        if not relayed or p != last:
            return jnp.bool_(False)
        source = jnp.where(z == 0, 1, jnp.where(z == Z - 1, Z - 2, jnp.where(z < Z // 2, z - 1, z + 1)))
        return q == source

    def relay(way):
        device = (up_dev, dn_dev)[way]
        block_there = block_at(z, 1 - x, last)
        return remote(block_there, block_there, relay_s.at[way], gat_r.at[z, 1 - x, last], device)

    def relays_to_ends(f):
        if relayed:
            @pl.when(z == Z - 2)
            def _():
                f(relay(0))

            @pl.when(z == 1)
            def _():
                f(relay(1))

    def relays_inward(f):
        if relayed:
            @pl.when(z + 1 < Z // 2)
            def _():
                f(relay(0))

            @pl.when((z - 1 >= Z // 2) & (z >= 1))
            def _():
                f(relay(1))

    def pass_on(q, ways, p):
        if 0 in ways:
            @pl.when(has_up)
            def _():
                hop(q, 0, p).start()

        if 1 in ways:
            @pl.when(has_dn)
            def _():
                hop(q, 1, p).start()

        @pl.when(jnp.logical_not(skips_x(q, p)))
        def _():
            hop(q, 2, p).start()

    for p in range(pieces):
        pass_on(z, (0, 1), p)
    weights_copy = remote(weight_ref, wother, send_sem.at[0], recv_sem.at[0], c_dev)
    weights_copy.start()
    for copy in right_loads:
        copy.start()

    depth = X * rows
    planewise = depth % PLANE_DEPTH == 0
    tile = min(ROW_TILE, block)
    tiles = block // tile

    def multiply(q, stage):
        plane = wbuf.at[q]

        def one(i, carry):
            k, at = i // tiles, pl.multiple_of(lax.rem(i, tiles) * tile, tile)
            cols = pl.ds(pl.multiple_of(q * depth, depth), depth)
            product = jnp.dot(
                lbuf[k, pl.ds(at, tile), cols], plane[...].reshape(depth, block), preferred_element_type=F32
            )
            if stage == "only":
                left[k, pl.ds(at, tile), :] = product.astype(BF16)
            elif stage == "first":
                acc[k, pl.ds(at, tile), :] = product
            elif stage == "middle":
                acc[k, pl.ds(at, tile), :] += product
            else:
                left[k, pl.ds(at, tile), :] = (acc[k, pl.ds(at, tile), :] + product).astype(BF16)
            return carry

        lax.fori_loop(0, K * tiles, one, 0)

    def take_plane(q, stage):
        for p in range(pieces):
            arrival(q, 1 - x, p).wait_recv()
        if stage == "first":
            relays_inward(lambda copy: copy.start())
        if planewise:
            multiply(q, stage)

    pltpu.make_async_copy(lbuf, lbuf, load_sem.at[0]).wait()

    def forward(d, carry):
        lo, hi = z - d, z + d
        for p in range(pieces):
            @pl.when(lo >= 0)
            def _():
                arrival(lo, x, p).wait_recv()
                pass_on(lo, (0,), p)

            @pl.when(hi < Z)
            def _():
                arrival(hi, x, p).wait_recv()
                pass_on(hi, (1,), p)

        @pl.when(d == 1)
        def _():
            take_plane(z, "first")

        return carry

    if Z == 1:
        take_plane(z, "only")
    lax.fori_loop(1, Z, forward, 0)
    relays_to_ends(lambda copy: copy.start())
    near = jnp.minimum(z, Z - 1 - z)

    def plane_by_distance(i):
        d = (i + 1) // 2
        both = jnp.where(lax.rem(i, 2) == 1, z - d, z + d)
        return jnp.where(i <= 2 * near, both, jnp.where(z > near, z - (i - near), z + (i - near)))

    def take_planes(i, carry):
        take_plane(plane_by_distance(i), "middle")
        return carry

    lax.fori_loop(1, Z - 1, take_planes, 0)
    if Z > 1:
        take_plane(plane_by_distance(jnp.int32(Z - 1)), "last")

    def whole_left(i, carry):
        k, at = i // tiles, pl.multiple_of(lax.rem(i, tiles) * tile, tile)
        value = jnp.dot(
            lbuf[k, pl.ds(at, tile), :], wbuf[...].reshape(block, block), preferred_element_type=F32
        )
        left[k, pl.ds(at, tile), :] = value.astype(BF16)
        return carry

    if not planewise:
        lax.fori_loop(0, K * tiles, whole_left, 0)
    pltpu.make_async_copy(rbuf, rbuf, load_sem.at[1]).wait()

    def core_copy(g, k):
        return remote(psend.at[g, k], precv.at[g, k], send_sem.at[1], recv_sem.at[1 + g], c_dev)

    def core_arrival(g):
        return remote(psend.at[g], precv.at[g], send_sem.at[1], recv_sem.at[1 + g], c_dev)

    def second(g, k):
        def one(i, carry):
            at = pl.multiple_of(i * tile, tile)
            term = lax.dot_general(
                left[k, pl.ds(at, tile), :], rbuf[k, g].reshape(2 * LANES, block),
                (((1,), (1,)), ((), ())), preferred_element_type=F32,
            )
            psend[g, k, pl.ds(at, tile), :] = term[:, :LANES].astype(BF16)
            own[g, k, pl.ds(at, tile), :] = term[:, LANES:]
            return carry

        lax.fori_loop(0, tiles, one, 0)
        core_copy(g, k).start()

    def chip_sum(n, ty, zz, xx):
        unit = units[n]
        at = pl.ds(pl.multiple_of((zz * X + xx) * rows + unit.start, unit.count), unit.count)
        t = ty * 2 + unit.core
        total = None
        for k in range(K):
            mine = own[unit.group, k, at, :] * weight_ref[k * T + t, 0:1, :]
            theirs = precv[unit.group, k, at, :].astype(F32) * wother[k * T + t, 0:1, :]
            total = mine + theirs if total is None else total + mine + theirs
        return total

    def put_x(n, index, value):
        xs[rows_of(n, 0, index), :] = value.astype(BF16)

    def put_y(n, index, value):
        ys[rows_of(n, 1, index), :] = value.astype(BF16)

    def put_z(n, index, value):
        zs[rows_of(n, 2, index), :] = value.astype(BF16)

    def from_x(n, index):
        return xr[rows_of(n, 0, index), :].astype(F32)

    def from_y(n, index):
        return yr[rows_of(n, 1, index), :].astype(F32)

    def from_z(n, index):
        return zr[rows_of(n, 2, index), :].astype(F32)

    def step_copy(n, letter, slot):
        axis = "xy".index(letter)
        s, r = ((xs, xr), (ys, yr))[axis]
        span = pl.ds(offsets[n][axis], unit_sizes(units[n], Z, X)[axis] * units[n].count)
        device = (x_dev, y_dev)[axis]
        return remote(s.at[span], r.at[span], send_sem.at[2 + axis], pair_sem.at[pair_of[n], slot], device)

    def z_span(n, zz):
        size = unit_sizes(units[n], Z, X)[2] // Z * units[n].count
        return pl.ds(pl.multiple_of(offsets[n][2] + zz * size, units[n].count), size)

    def line_slot(n):
        return 2 if units[n].order[2] == "z" else 0

    def line_copy(n, zz):
        sem = pair_sem.at[pair_of[n], line_slot(n)]
        return remote(zs.at[z_span(n, zz)], zr.at[z_span(n, z)], send_sem.at[4], sem, dev(zz=zz))

    def wait_rows(sem, count):
        if count:
            pltpu.make_async_copy(zs.at[pl.ds(0, count)], zs.at[pl.ds(0, count)], sem).wait()

    def wait_pair(i, slot):
        count = 0
        for n in numbers[i]:
            unit, sizes = units[n], unit_sizes(units[n], Z, X)
            letter = unit.order[slot]
            count += (sizes["xyz".index(letter)] // Z * (Z - 1) if letter == "z" else sizes["xyz".index(letter)]) * unit.count
        wait_rows(pair_sem.at[i, slot], count)

    def others(f):
        loop(Z - 1, lambda j: f(lax.rem(z + 1 + j, Z)))

    def send(n):
        order = units[n].order
        if order == "xyz":
            def one(zz):
                for ty in range(2):
                    put_x(n, ty * Z + zz, chip_sum(n, ty, zz, 1 - x))

            loop(Z, one)
            step_copy(n, "x", 0).start()
        elif order == "yxz":
            def one(zz):
                for xx in range(X):
                    put_y(n, zz * X + xx, chip_sum(n, 1 - y, zz, xx))

            loop(Z, one)
            step_copy(n, "y", 0).start()
        else:
            def one(zz):
                for ty in range(2):
                    for xx in range(X):
                        put_z(n, z_index(n, zz, ty, xx), chip_sum(n, ty, zz, xx))
                line_copy(n, zz).start()

            others(one)

    def line_sum(n, value, ty=0, xx=0):
        if Z <= 8:
            for zz in range(Z):
                value = value + from_z(n, z_index(n, zz, ty, xx))
            return value
        return lax.fori_loop(0, Z, lambda zz, v: v + from_z(n, z_index(n, zz, ty, xx)), value)

    def summed(n, ty, xx):
        return line_sum(n, chip_sum(n, ty, z, xx), ty, xx)

    def send_again(n):
        order = units[n].order
        if order == "xyz":
            def one(zz):
                put_y(n, zz, chip_sum(n, 1 - y, zz, x) + from_x(n, (1 - y) * Z + zz))

            loop(Z, one)
        elif order == "yxz":
            def one(zz):
                put_x(n, zz, chip_sum(n, y, zz, 1 - x) + from_y(n, zz * X + 1 - x))

            loop(Z, one)
        else:
            for j in range(2):
                if order == "zxy":
                    put_x(n, j, summed(n, j, 1 - x))
                else:
                    put_y(n, j, summed(n, 1 - y, j))
        step_copy(n, order[1], 1).start()

    def plane_sum(n, zz):
        value = chip_sum(n, y, zz, x)
        if units[n].order == "xyz":
            return value + from_x(n, y * Z + zz) + from_y(n, zz)
        return value + from_y(n, zz * X + x) + from_x(n, zz)

    def send_last(n):
        order = units[n].order
        if order[2] == "z":
            def one(zz):
                put_z(n, zz, plane_sum(n, zz))
                line_copy(n, zz).start()

            others(one)
        elif order == "zxy":
            put_y(n, 0, summed(n, 1 - y, x) + from_x(n, 1 - y))
            step_copy(n, "y", 2).start()
        else:
            put_x(n, 0, summed(n, y, 1 - x) + from_y(n, 1 - x))
            step_copy(n, "x", 2).start()

    def total(n):
        order = units[n].order
        if order[2] == "z":
            return line_sum(n, plane_sum(n, z))
        if order == "zxy":
            return summed(n, y, x) + from_x(n, y) + from_y(n, 0)
        return summed(n, y, x) + from_y(n, x) + from_x(n, 0)

    def final_copy(g):
        return remote(fsend.at[g], frecv.at[g], send_sem.at[5], recv_sem.at[1 + groups + g], c_dev)

    numbers, pair_of = [], {}
    for i, members in enumerate(pairs):
        numbers.append([units.index(unit) for unit in members])
        for n in numbers[i]:
            pair_of[n] = i

    def finish(g):
        at = pl.multiple_of(c * half + g * LANES, LANES)
        for i in range(len(pairs)):
            if units[numbers[i][0]].group == g:
                wait_pair(i, 2)
        here = [n for n in range(len(units)) if units[n].group == g]
        for n in here:
            if units[n].core == 0:
                start, count = units[n].start, units[n].count
                twin = [m for m in here if units[m].core == 1 and units[m].start == start]
                one, two = total(n), total(twin[0])
                span = pl.ds(start, count)
                out_ref[span, pl.ds(at, LANES)] = jnp.where(c == 0, one, two) * used(at, start, count)
                fsend[g, span, :] = jnp.where(c == 0, two, one)
        final_copy(g).start()

    def each(f, i):
        for n in numbers[i]:
            f(n)

    ready = set()

    def receive(g):
        if g not in ready:
            ready.add(g)
            core_arrival(g).wait_recv()

    queue = [(g, k) for g in range(groups) for k in range(K)]

    def compute(count):
        for _ in range(min(count, len(queue))):
            second(*queue.pop(0))

    def start_pair(i):
        g = units[numbers[i][0]].group
        while queue and queue[0][0] <= g:
            compute(1)
        receive(g)
        each(send, i)

    turned = 1
    plain = [i for i in range(len(pairs)) if i != turned]
    steps = len(plain)
    done = set()
    compute(K + 1)
    weights_copy.wait_recv()
    start_pair(plain[0])
    start_pair(turned)
    start_pair(plain[1])
    compute(K)
    for j in range(steps):
        wait_pair(plain[j], 0)
        each(send_again, plain[j])
        if j + 2 < steps:
            start_pair(plain[j + 2])
            compute(1)
        if j == max(0, steps - 3):
            wait_pair(turned, 0)
            each(send_again, turned)
        if j == steps - 1:
            wait_pair(turned, 1)
            each(send_last, turned)
        if j >= 1:
            wait_pair(plain[j - 1], 1)
            each(send_last, plain[j - 1])
        if j >= steps - 2 and 1 + j - (steps - 2) < groups - 1:
            finish(1 + j - (steps - 2))
            done.add(1 + j - (steps - 2))
    wait_pair(plain[steps - 1], 1)
    each(send_last, plain[steps - 1])
    for g in (*range(1, groups - 1), 0, groups - 1):
        if g not in done:
            done.add(g)
            finish(g)
    for g in range(groups):
        final_copy(g).wait_recv()
        at = pl.multiple_of((1 - c) * half + g * LANES, LANES)
        out_ref[:, pl.ds(at, LANES)] = frecv[g] * used(at)

    for v in range(Z):
        @pl.when(z == v)
        def _(v=v):
            for way, count in ((0, v + 1 if v + 1 < Z else 0), (1, Z - v if v else 0)):
                if count:
                    span = wbuf.at[pl.ds(0, count), 0]
                    pltpu.make_async_copy(span, span, gat_s.at[way]).wait()

    count = Z * rows - (piece if relayed else 0)
    flat = left.at[0, pl.ds(0, count)]
    pltpu.make_async_copy(flat, flat, gat_s.at[2]).wait()
    relays_to_ends(lambda copy: copy.wait_send())
    relays_inward(lambda copy: copy.wait_send())
    weights_copy.wait_send()
    pltpu.make_async_copy(psend, psend, send_sem.at[1]).wait()
    pltpu.make_async_copy(xs, xs, send_sem.at[2]).wait()
    pltpu.make_async_copy(ys, ys, send_sem.at[3]).wait()
    wait_rows(send_sem.at[4], zs.shape[0] // Z * (Z - 1))
    pltpu.make_async_copy(fsend, fsend, send_sem.at[5]).wait()


def body(wave, left_ops, right_ops, targets, sector_sizes, pair_ids, pair_coefficients):
    block = wave.shape[2]
    rows = wave.shape[1]
    K = left_ops.shape[0]
    T = sector_sizes.shape[0]
    X = 2
    Z = lax.axis_size("pair") // X
    groups = block // 2 // LANES
    pairs = plan(groups, rows)
    heights = [0, 0, 0]
    for pair in pairs:
        for unit in pair:
            heights = [height + size * unit.count for height, size in zip(heights, unit_sizes(unit, Z, X))]
    dma = pltpu.SemaphoreType.DMA
    planewise = (X * rows) % PLANE_DEPTH == 0
    hbm = pl.BlockSpec(memory_space=pltpu.HBM)
    operands = (
        wave[0], targets.reshape(-1), sector_sizes, pair_ids, pair_coefficients, left_ops[:, 0], right_ops[:, 0]
    )
    out = pl.pallas_call(
        functools.partial(step_kernel, (Z, X, T, K, rows, block, groups, pairs)),
        out_shape=jax.ShapeDtypeStruct((rows, block), F32),
        in_specs=[hbm] * 7,
        out_specs=pl.BlockSpec(memory_space=pltpu.VMEM),
        scratch_shapes=[
            *(pltpu.SMEM(a.shape, a.dtype) for a in operands[1:5]),
            pltpu.VMEM((rows, block), BF16),
            pltpu.VMEM((Z, X, rows, block), BF16),
            pltpu.VMEM((K, block, block), BF16),
            pltpu.VMEM((K, groups, 2, LANES, block), BF16),
            pltpu.VMEM((K, block, block) if planewise else (8, LANES), F32),
            pltpu.VMEM((K, block, block), BF16),
            pltpu.VMEM((groups, K, block, LANES), F32),
            pltpu.VMEM((groups, K, block, LANES), BF16),
            pltpu.VMEM((groups, K, block, LANES), BF16),
            pltpu.VMEM((K * T, 8, LANES), F32),
            pltpu.VMEM((K * T, 8, LANES), F32),
            pltpu.VMEM((groups, rows, LANES), F32),
            pltpu.VMEM((groups, rows, LANES), F32),
            *(pltpu.VMEM((height, LANES), BF16) for height in heights for _ in range(2)),
            dma((7,)), dma((6,)), dma((1 + 2 * groups,)), dma((len(pairs), 3)),
            dma((3,)), dma((Z, X, PIECES)), dma((2,)),
        ],
        compiler_params=pltpu.CompilerParams(
            collective_id=0, has_side_effects=True, vmem_limit_bytes=VMEM_LIMIT
        ),
        name="sigma_step",
    )(*(pltpu.with_memory_space_constraint(a, pltpu.HBM) for a in operands))
    return out[None]


def solution(mesh):
    placed = (
        P("sector", "pair", None),
        P("pair", "sector", None, None),
        P("pair", "sector", None, None),
        P("pair", "sector"),
        P(),
        P("pair"),
        P(),
    )
    return jax.shard_map(
        body, mesh=mesh, in_specs=placed, out_specs=P("sector", "pair", None), check_vma=False
    )
```

```python
import functools

import jax
import jax.numpy as jnp
from jax import lax
from jax.experimental import pallas as pl
from jax.experimental.pallas import tpu as pltpu
from jax.sharding import PartitionSpec as P

MESH = pl.DeviceIdType.MESH
F32 = jnp.float32
BF16 = jnp.bfloat16
LANES = 128
ROW_TILE = 1024
PIECES = 4
VMEM_LIMIT = 48 * 1024 * 1024


class Unit:
    def __init__(self, group, core, start, count, order):
        self.group, self.core, self.start, self.count, self.order = group, core, start, count, order


def plan(groups, rows):
    pairs = []
    for g in range(groups):
        parts = 1 if rows % 32 else 4 if g == groups - 1 and rows % 64 == 0 else 2
        count = rows // parts
        if parts == 1:
            found = [[(g, tc, 0, rows) for tc in range(2)]]
        else:
            found = [
                [(g, tc, (i + h) * count, count) for h in range(2)] for tc in range(2) for i in range(0, parts, 2)
            ]
        pairs += found
    orders = [("zxy", "zyx") if n == 1 else ("xyz", "yxz") for n in range(len(pairs))]
    return [[Unit(*part, order) for part, order in zip(pair, way)] for pair, way in zip(pairs, orders)]


def unit_sizes(unit, Z, X):
    return {
        "xyz": (2 * Z, Z, Z),
        "yxz": (Z, Z * X, Z),
        "zxy": (2, 1, Z * 2 * X),
        "zyx": (1, X, Z * 2 * X),
    }[unit.order]


def step_kernel(
    cfg, wave_hbm, targets_hbm, sizes_hbm, ids_hbm, coefs_hbm, left_hbm, right_hbm, out_ref,
    targets_ref, sizes_ref, ids_ref, coefs_ref,
    wave_ref, wbuf, lbuf, rbuf, acc, first_acc, left, own, psend, precv, weight_ref, wother, fsend, frecv,
    xs, xr, ys, yr, zs, zr, load_sem, send_sem, recv_sem, pair_sem, gat_s, gat_r, relay_s,
):
    Z, X, T, K, rows, block, groups, pairs = cfg
    units = [unit for pair in pairs for unit in pair]
    offsets, ends = [], [0, 0, 0]
    for unit in units:
        offsets.append(tuple(ends))
        ends = [end + size * unit.count for end, size in zip(ends, unit_sizes(unit, Z, X))]
    half = block // 2
    pair, sector = lax.axis_index("pair"), lax.axis_index("sector")
    z, x = pair // X, lax.rem(pair, X)
    y, c = sector // 2, lax.rem(sector, 2)

    def dev(zz=None, xx=None, yy=None, cc=None):
        zz, xx = z if zz is None else zz, x if xx is None else xx
        yy, cc = y if yy is None else yy, c if cc is None else cc
        return (zz * X + xx, yy * 2 + cc)

    x_dev, y_dev, c_dev = dev(xx=1 - x), dev(yy=1 - y), dev(cc=1 - c)
    up_dev, dn_dev = dev(zz=z + 1), dev(zz=z - 1)

    def loop(count, f):
        def one(i, carry):
            f(i)
            return carry

        lax.fori_loop(0, count, one, 0)

    has_up, has_dn = z + 1 < Z, z >= 1
    nested = Z == 4 and rows % LANES == 0
    pieces = PIECES
    width = block // pieces
    late = range(pieces // 2, pieces) if nested else ()

    left_loads = [pltpu.make_async_copy(left_hbm.at[k], lbuf.at[k], load_sem.at[0]) for k in range(K)]
    right_loads = []
    for k in range(K):
        for g in range(groups):
            for j in range(2):
                at = pl.multiple_of((1 - c if j == 0 else c) * half + g * LANES, LANES)
                right_loads.append(
                    pltpu.make_async_copy(
                        right_hbm.at[k, pl.ds(at, LANES)], rbuf.at[k, g, j],
                        load_sem.at[1],
                    )
                )

    barrier = pltpu.get_barrier_semaphore()
    for other in (x_dev, y_dev, c_dev):
        pl.semaphore_signal(barrier, inc=1, device_id=other, device_id_type=MESH)

    wave_load = pltpu.make_async_copy(wave_hbm, wave_ref, load_sem.at[2])
    wave_load.start()
    small_loads = [
        pltpu.make_async_copy(src, dst, load_sem.at[3 + i])
        for i, (src, dst) in enumerate(
            ((targets_hbm, targets_ref), (sizes_hbm, sizes_ref), (ids_hbm, ids_ref), (coefs_hbm, coefs_ref))
        )
    ]
    for copy in small_loads:
        copy.start()

    @pl.when(has_up)
    def _():
        pl.semaphore_signal(barrier, inc=1, device_id=up_dev, device_id_type=MESH)

    @pl.when(has_dn)
    def _():
        pl.semaphore_signal(barrier, inc=1, device_id=dn_dev, device_id_type=MESH)

    def rows_of(n, axis, index):
        count = units[n].count
        return pl.ds(pl.multiple_of(offsets[n][axis] + index * count, count), count)

    def z_index(n, zz, ty=0, xx=0):
        return zz if units[n].order[2] == "z" else (zz * 2 + ty) * X + xx

    for n, unit in enumerate(units):
        size = unit_sizes(unit, Z, X)[2] // Z * unit.count
        zr[pl.ds(pl.multiple_of(offsets[n][2] + z * size, unit.count), size), :] = jnp.zeros((size, LANES), BF16)
    for copy in left_loads:
        copy.start()
    for copy in small_loads:
        copy.wait()
    for k in range(K):
        factor = coefs_ref[ids_ref[k]]
        for t in range(T):
            chosen = jnp.where(targets_ref[k] == t, factor, 0.0)
            weight_ref[k * T + t] = jnp.full((8, LANES), chosen, F32)
    size = sizes_ref[sector]

    def used(column, start=0, count=rows):
        row_ids = pair * rows + start + lax.broadcasted_iota(jnp.int32, (count, LANES), 0)
        lane_ids = column + lax.broadcasted_iota(jnp.int32, (count, LANES), 1)
        return ((row_ids < size) & (lane_ids < size)).astype(F32)

    wave_load.wait()
    for at in range(0, block, LANES):
        value = wave_ref[:, at : at + LANES].astype(F32) * used(at)
        p = at // width
        where = (x, p, z) if nested else (p, z, x)
        wbuf[(*where, slice(None), slice(at - p * width, at - p * width + LANES))] = value.astype(BF16)
    pl.semaphore_wait(barrier, 3 + has_up.astype(jnp.int32) + has_dn.astype(jnp.int32))

    def remote(src, dst, ss, rs, device):
        return pltpu.make_async_remote_copy(
            src_ref=src, dst_ref=dst, send_sem=ss, recv_sem=rs, device_id=device, device_id_type=MESH
        )

    def block_at(q, xx, p):
        return wbuf.at[(xx, p, q) if nested else (p, q, xx)]

    def hop(q, way, p):
        device = (up_dev, dn_dev, x_dev)[way]
        return remote(block_at(q, x, p), block_at(q, x, p), gat_s.at[way], gat_r.at[q, x, p], device)

    def arrival(q, xx, p):
        return remote(block_at(q, xx, p), block_at(q, xx, p), gat_s.at[2], gat_r.at[q, xx, p], x_dev)

    def skips_x(q, p):
        if p not in late:
            return jnp.bool_(False)
        return q == jnp.where(z == 0, 2, jnp.where(z == 1, 0, jnp.where(z == 2, 3, 1)))

    def relay(q, way):
        for p in late:
            block_there = block_at(q, 1 - x, p)
            remote(block_there, block_there, relay_s.at[0], gat_r.at[q, 1 - x, p], (up_dev, dn_dev)[way]).start()

    def relay_when(where, q, way):
        @pl.when(z == where)
        def _():
            relay(q, way)

    def pass_on(q, ways, p):
        if 0 in ways:
            @pl.when(has_up)
            def _():
                hop(q, 0, p).start()

        if 1 in ways:
            @pl.when(has_dn)
            def _():
                hop(q, 1, p).start()

        @pl.when(jnp.logical_not(skips_x(q, p)))
        def _():
            hop(q, 2, p).start()

    for p in range(pieces):
        pass_on(z, (0, 1), p)
    weights_copy = remote(weight_ref, wother, send_sem.at[0], recv_sem.at[0], c_dev)
    weights_copy.start()
    for copy in right_loads:
        copy.start()

    tile = min(ROW_TILE, block)
    tiles = block // tile

    def multiply(j, xx, ps, stage, ks=tuple(range(K))):
        def one(i, carry):
            k, at = ks[0] + i // tiles, pl.multiple_of(lax.rem(i, tiles) * tile, tile)
            sides = [
                lbuf[k, pl.ds(at, tile), pl.ds(pl.multiple_of(((2 * j + n) * X + xx) * rows, rows), rows)]
                for n in range(2)
            ]
            both = jnp.concatenate(sides, axis=1)
            for p in ps:
                product = jnp.dot(
                    both, wbuf[xx, p, pl.ds(2 * j, 2)].reshape(2 * rows, width), preferred_element_type=F32
                )
                if stage == "first":
                    acc[k, p, pl.ds(at, tile), :] = product
                elif stage == "middle":
                    acc[k, p, pl.ds(at, tile), :] += product
                else:
                    left[k, pl.ds(at, tile), pl.ds(p * width, width)] = (
                        acc[k, p, pl.ds(at, tile), :] + product
                    ).astype(BF16)
            return carry

        lax.fori_loop(0, len(ks) * tiles, one, 0)

    def split_term(g, k, at, term):
        psend[g, k, pl.ds(at, tile), :] = term[:, :LANES].astype(BF16)
        own[g, k, pl.ds(at, tile), :] = term[:, LANES:]

    def core_copy(g, k):
        return remote(psend.at[g, k], precv.at[g, k], send_sem.at[1], recv_sem.at[1 + g], c_dev)

    def first_second(h):
        cols = pl.ds(h * block // 2, block // 2)

        def one(i, carry):
            at = pl.multiple_of(i * tile, tile)
            for k in range(K):
                term = lax.dot_general(
                    left[k, pl.ds(at, tile), cols], rbuf[k, 0, :, :, cols].reshape(2 * LANES, block // 2),
                    (((1,), (1,)), ((), ())), preferred_element_type=F32,
                )
                if h == 0:
                    first_acc[k, pl.ds(at, tile), :] = term
                else:
                    split_term(0, k, at, first_acc[k, pl.ds(at, tile), :] + term)
            return carry

        lax.fori_loop(0, tiles, one, 0)
        if h == 1:
            for k in range(K):
                core_copy(0, k).start()

    def forward(d, p):
        lo, hi = z - d, z + d

        @pl.when(lo >= 0)
        def _():
            arrival(lo, x, p).wait_recv()
            pass_on(lo, (0,), p)

        @pl.when(hi < Z)
        def _():
            arrival(hi, x, p).wait_recv()
            pass_on(hi, (1,), p)

    def mirrored(q):
        for p in range(pieces):
            arrival(q, 1 - x, p).wait_recv()

    pltpu.make_async_copy(lbuf, lbuf, load_sem.at[0]).wait()
    if nested:
        near = z // 2
        far = 1 - near
        far_first = jnp.where(near == 0, 2, 1)
        for p in range(pieces):
            forward(1, p)
        mirrored(z)
        relay_when(0, 0, 0)
        relay_when(3, 3, 1)
        every = tuple(range(pieces))
        halves = every[: pieces // 2], every[pieces // 2 :]
        multiply(near, x, every, "first")
        for p in every:
            forward(2, p)
        mirrored(4 * near + 1 - z)
        for k in range(K):
            multiply(near, 1 - x, every, "middle", (k,))
            if k < 2:
                for p in halves[0][k :: 2]:
                    forward(3, p)
        multiply(far, x, halves[0], "middle")
        for p in halves[1]:
            forward(3, p)
        multiply(far, x, halves[1], "middle")
        inner = (z == 1) | (z == 2)

        @pl.when(inner)
        def _():
            mirrored(far_first)

        relay_when(1, 2, 1)
        relay_when(2, 1, 0)
        pltpu.make_async_copy(rbuf, rbuf, load_sem.at[1]).wait()
        for h in range(2):
            @pl.when(jnp.logical_not(inner))
            def _(h=h):
                for p in halves[h]:
                    arrival(far_first, 1 - x, p).wait_recv()

            for p in halves[h]:
                arrival(4 * far + 1 - far_first, 1 - x, p).wait_recv()
            multiply(far, 1 - x, halves[h], "last")
            first_second(h)
    else:
        def forward_all(d, carry):
            for p in range(pieces):
                forward(d, p)
            return carry

        def mirrored_all(q, carry):
            mirrored(q)
            return carry

        def whole_left(i, carry):
            k, at = i // tiles, pl.multiple_of(lax.rem(i, tiles) * tile, tile)
            for p in range(pieces):
                value = jnp.dot(
                    lbuf[k, pl.ds(at, tile), :], wbuf[p].reshape(block, width), preferred_element_type=F32
                )
                left[k, pl.ds(at, tile), pl.ds(p * width, width)] = value.astype(BF16)
            return carry

        lax.fori_loop(1, Z, forward_all, 0)
        lax.fori_loop(0, Z, mirrored_all, 0)
        lax.fori_loop(0, K * tiles, whole_left, 0)
        pltpu.make_async_copy(rbuf, rbuf, load_sem.at[1]).wait()

    def core_arrival(g):
        return remote(psend.at[g], precv.at[g], send_sem.at[1], recv_sem.at[1 + g], c_dev)

    def second(g):
        def one(i, carry):
            at = pl.multiple_of(i * tile, tile)
            for k in range(K):
                term = lax.dot_general(
                    left[k, pl.ds(at, tile), :], rbuf[k, g].reshape(2 * LANES, block),
                    (((1,), (1,)), ((), ())), preferred_element_type=F32,
                )
                split_term(g, k, at, term)
            return carry

        lax.fori_loop(0, tiles, one, 0)
        for k in range(K):
            core_copy(g, k).start()

    def chip_sum(n, ty, zz, xx):
        unit = units[n]
        at = pl.ds(pl.multiple_of((zz * X + xx) * rows + unit.start, unit.count), unit.count)
        t = ty * 2 + unit.core
        total = None
        for k in range(K):
            mine = own[unit.group, k, at, :] * weight_ref[k * T + t, 0:1, :]
            theirs = precv[unit.group, k, at, :].astype(F32) * wother[k * T + t, 0:1, :]
            total = mine + theirs if total is None else total + mine + theirs
        return total

    def put_x(n, index, value):
        xs[rows_of(n, 0, index), :] = value.astype(BF16)

    def put_y(n, index, value):
        ys[rows_of(n, 1, index), :] = value.astype(BF16)

    def put_z(n, index, value):
        zs[rows_of(n, 2, index), :] = value.astype(BF16)

    def from_x(n, index):
        return xr[rows_of(n, 0, index), :].astype(F32)

    def from_y(n, index):
        return yr[rows_of(n, 1, index), :].astype(F32)

    def from_z(n, index):
        return zr[rows_of(n, 2, index), :].astype(F32)

    def step_copy(n, letter, slot):
        axis = "xy".index(letter)
        s, r = ((xs, xr), (ys, yr))[axis]
        span = pl.ds(offsets[n][axis], unit_sizes(units[n], Z, X)[axis] * units[n].count)
        device = (x_dev, y_dev)[axis]
        return remote(s.at[span], r.at[span], send_sem.at[2 + axis], pair_sem.at[pair_of[n], slot], device)

    def z_span(n, zz):
        size = unit_sizes(units[n], Z, X)[2] // Z * units[n].count
        return pl.ds(pl.multiple_of(offsets[n][2] + zz * size, units[n].count), size)

    def line_slot(n):
        return 2 if units[n].order[2] == "z" else 0

    def line_copy(n, zz):
        sem = pair_sem.at[pair_of[n], line_slot(n)]
        return remote(zs.at[z_span(n, zz)], zr.at[z_span(n, z)], send_sem.at[4], sem, dev(zz=zz))

    def wait_rows(sem, count):
        if count:
            pltpu.make_async_copy(zs.at[pl.ds(0, count)], zs.at[pl.ds(0, count)], sem).wait()

    def wait_pair(i, slot):
        count = 0
        for n in numbers[i]:
            unit, sizes = units[n], unit_sizes(units[n], Z, X)
            letter = unit.order[slot]
            count += (sizes["xyz".index(letter)] // Z * (Z - 1) if letter == "z" else sizes["xyz".index(letter)]) * unit.count
        wait_rows(pair_sem.at[i, slot], count)

    def others(f):
        loop(Z - 1, lambda j: f(lax.rem(z + 1 + j, Z)))

    def send(n):
        order = units[n].order
        if order == "xyz":
            def one(zz):
                for ty in range(2):
                    put_x(n, ty * Z + zz, chip_sum(n, ty, zz, 1 - x))

            loop(Z, one)
            step_copy(n, "x", 0).start()
        elif order == "yxz":
            def one(zz):
                for xx in range(X):
                    put_y(n, zz * X + xx, chip_sum(n, 1 - y, zz, xx))

            loop(Z, one)
            step_copy(n, "y", 0).start()
        else:
            def one(zz):
                for ty in range(2):
                    for xx in range(X):
                        put_z(n, z_index(n, zz, ty, xx), chip_sum(n, ty, zz, xx))
                line_copy(n, zz).start()

            others(one)

    def line_sum(n, value, ty=0, xx=0):
        if Z <= 8:
            for zz in range(Z):
                value = value + from_z(n, z_index(n, zz, ty, xx))
            return value
        return lax.fori_loop(0, Z, lambda zz, v: v + from_z(n, z_index(n, zz, ty, xx)), value)

    def summed(n, ty, xx):
        return line_sum(n, chip_sum(n, ty, z, xx), ty, xx)

    def send_again(n):
        order = units[n].order
        if order == "xyz":
            def one(zz):
                put_y(n, zz, chip_sum(n, 1 - y, zz, x) + from_x(n, (1 - y) * Z + zz))

            loop(Z, one)
        elif order == "yxz":
            def one(zz):
                put_x(n, zz, chip_sum(n, y, zz, 1 - x) + from_y(n, zz * X + 1 - x))

            loop(Z, one)
        else:
            for j in range(2):
                if order == "zxy":
                    put_x(n, j, summed(n, j, 1 - x))
                else:
                    put_y(n, j, summed(n, 1 - y, j))
        step_copy(n, order[1], 1).start()

    def plane_sum(n, zz):
        value = chip_sum(n, y, zz, x)
        if units[n].order == "xyz":
            return value + from_x(n, y * Z + zz) + from_y(n, zz)
        return value + from_y(n, zz * X + x) + from_x(n, zz)

    def send_last(n):
        order = units[n].order
        if order[2] == "z":
            def one(zz):
                put_z(n, zz, plane_sum(n, zz))
                line_copy(n, zz).start()

            others(one)
        elif order == "zxy":
            put_y(n, 0, summed(n, 1 - y, x) + from_x(n, 1 - y))
            step_copy(n, "y", 2).start()
        else:
            put_x(n, 0, summed(n, y, 1 - x) + from_y(n, 1 - x))
            step_copy(n, "x", 2).start()

    def total(n):
        order = units[n].order
        if order[2] == "z":
            return line_sum(n, plane_sum(n, z))
        if order == "zxy":
            return summed(n, y, x) + from_x(n, y) + from_y(n, 0)
        return summed(n, y, x) + from_y(n, x) + from_x(n, 0)

    def final_copy(g):
        return remote(fsend.at[g], frecv.at[g], send_sem.at[5], recv_sem.at[1 + groups + g], c_dev)

    numbers, pair_of = [], {}
    for i, members in enumerate(pairs):
        numbers.append([units.index(unit) for unit in members])
        for n in numbers[i]:
            pair_of[n] = i

    def finish(g):
        at = pl.multiple_of(c * half + g * LANES, LANES)
        for i in range(len(pairs)):
            if units[numbers[i][0]].group == g:
                wait_pair(i, 2)
        here = [n for n in range(len(units)) if units[n].group == g]
        for n in here:
            if units[n].core == 0:
                start, count = units[n].start, units[n].count
                twin = [m for m in here if units[m].core == 1 and units[m].start == start]
                one, two = total(n), total(twin[0])
                span = pl.ds(start, count)
                out_ref[span, pl.ds(at, LANES)] = jnp.where(c == 0, one, two) * used(at, start, count)
                fsend[g, span, :] = jnp.where(c == 0, two, one)
        final_copy(g).start()

    def each(f, i):
        for n in numbers[i]:
            f(n)

    ready = set()

    def receive(g):
        if g not in ready:
            ready.add(g)
            core_arrival(g).wait_recv()

    queue = list(range(1 if nested else 0, groups))

    def compute(count):
        for _ in range(min(count, len(queue))):
            second(queue.pop(0))

    def start_pair(i):
        g = units[numbers[i][0]].group
        while queue and queue[0] <= g:
            compute(1)
        receive(g)
        each(send, i)

    turned = 1
    plain = [i for i in range(len(pairs)) if i != turned]
    steps = len(plain)
    done = set()
    compute(1 if nested else 2)
    weights_copy.wait_recv()
    start_pair(plain[0])
    start_pair(turned)
    start_pair(plain[1])
    compute(1)
    height = [units[numbers[i][0]].count for i in plain]
    following = 2
    for j in range(steps):
        wait_pair(plain[j], 0)
        each(send_again, plain[j])
        while following < steps and following < j + 4:
            start_pair(plain[following])
            following += 1
            compute(1)
        if j == steps - 1:
            wait_pair(turned, 0)
            each(send_again, turned)
        if j >= 1:
            wait_pair(plain[j - 1], 1)
            each(send_last, plain[j - 1])
        if j >= steps - 2 and 1 + j - (steps - 2) < groups - 1:
            finish(1 + j - (steps - 2))
            done.add(1 + j - (steps - 2))
    wait_pair(plain[steps - 1], 1)
    each(send_last, plain[steps - 1])
    wait_pair(turned, 1)
    each(send_last, turned)
    for g in (*range(1, groups - 1), 0, groups - 1):
        if g not in done:
            done.add(g)
            finish(g)
    for g in range(groups):
        final_copy(g).wait_recv()
        at = pl.multiple_of((1 - c) * half + g * LANES, LANES)
        out_ref[:, pl.ds(at, LANES)] = frecv[g] * used(at)

    for v in range(Z):
        @pl.when(z == v)
        def _(v=v):
            for way, count in ((0, v + 1 if v + 1 < Z else 0), (1, Z - v if v else 0)):
                if count:
                    span = left.at[0, pl.ds(0, count * rows)]
                    pltpu.make_async_copy(span, span, gat_s.at[way]).wait()

    count = Z * rows - len(late) * rows // pieces
    flat = left.at[0, pl.ds(0, count)]
    pltpu.make_async_copy(flat, flat, gat_s.at[2]).wait()
    if late:
        flat = left.at[0, pl.ds(0, len(late) * rows // pieces)]
        pltpu.make_async_copy(flat, flat, relay_s.at[0]).wait()
    weights_copy.wait_send()
    pltpu.make_async_copy(psend, psend, send_sem.at[1]).wait()
    pltpu.make_async_copy(xs, xs, send_sem.at[2]).wait()
    pltpu.make_async_copy(ys, ys, send_sem.at[3]).wait()
    wait_rows(send_sem.at[4], zs.shape[0] // Z * (Z - 1))
    pltpu.make_async_copy(fsend, fsend, send_sem.at[5]).wait()


def body(wave, left_ops, right_ops, targets, sector_sizes, pair_ids, pair_coefficients):
    block = wave.shape[2]
    rows = wave.shape[1]
    K = left_ops.shape[0]
    T = sector_sizes.shape[0]
    X = 2
    Z = lax.axis_size("pair") // X
    groups = block // 2 // LANES
    pairs = plan(groups, rows)
    heights = [0, 0, 0]
    for pair in pairs:
        for unit in pair:
            heights = [height + size * unit.count for height, size in zip(heights, unit_sizes(unit, Z, X))]
    dma = pltpu.SemaphoreType.DMA
    nested = Z == 4 and rows % LANES == 0
    width = block // PIECES
    hbm = pl.BlockSpec(memory_space=pltpu.HBM)
    operands = (
        wave[0], targets.reshape(-1), sector_sizes, pair_ids, pair_coefficients, left_ops[:, 0], right_ops[:, 0]
    )
    out = pl.pallas_call(
        functools.partial(step_kernel, (Z, X, T, K, rows, block, groups, pairs)),
        out_shape=jax.ShapeDtypeStruct((rows, block), F32),
        in_specs=[hbm] * 7,
        out_specs=pl.BlockSpec(memory_space=pltpu.VMEM),
        scratch_shapes=[
            *(pltpu.SMEM(a.shape, a.dtype) for a in operands[1:5]),
            pltpu.VMEM((rows, block), BF16),
            pltpu.VMEM((X, PIECES, Z, rows, width) if nested else (PIECES, Z, X, rows, width), BF16),
            pltpu.VMEM((K, block, block), BF16),
            pltpu.VMEM((K, groups, 2, LANES, block), BF16),
            pltpu.VMEM((K, PIECES, block, width) if nested else (8, LANES), F32),
            pltpu.VMEM((K, block, 2 * LANES) if nested else (8, LANES), F32),
            pltpu.VMEM((K, block, block), BF16),
            pltpu.VMEM((groups, K, block, LANES), F32),
            pltpu.VMEM((groups, K, block, LANES), BF16),
            pltpu.VMEM((groups, K, block, LANES), BF16),
            pltpu.VMEM((K * T, 8, LANES), F32),
            pltpu.VMEM((K * T, 8, LANES), F32),
            pltpu.VMEM((groups, rows, LANES), F32),
            pltpu.VMEM((groups, rows, LANES), F32),
            *(pltpu.VMEM((height, LANES), BF16) for height in heights for _ in range(2)),
            dma((7,)), dma((6,)), dma((1 + 2 * groups,)), dma((len(pairs), 3)),
            dma((3,)), dma((Z, X, PIECES)), dma((1,)),
        ],
        compiler_params=pltpu.CompilerParams(
            collective_id=0, has_side_effects=True, vmem_limit_bytes=VMEM_LIMIT
        ),
        name="sigma_step",
    )(*(pltpu.with_memory_space_constraint(a, pltpu.HBM) for a in operands))
    return out[None]


def solution(mesh):
    placed = (
        P("sector", "pair", None),
        P("pair", "sector", None, None),
        P("pair", "sector", None, None),
        P("pair", "sector"),
        P(),
        P("pair"),
        P(),
    )
    return jax.shard_map(
        body, mesh=mesh, in_specs=placed, out_specs=P("sector", "pair", None), check_vma=False
    )
```

```python
import functools

import jax
import jax.numpy as jnp
from jax import lax
from jax.experimental import pallas as pl
from jax.experimental.pallas import tpu as pltpu
from jax.sharding import PartitionSpec as P

MESH = pl.DeviceIdType.MESH
F32 = jnp.float32
BF16 = jnp.bfloat16
LANES = 128
ROW_TILE = 1024
PIECES = 4
VMEM_LIMIT = 48 * 1024 * 1024
TURNED = (1, 3)
MERGE_LAG = 3


class Unit:
    def __init__(self, group, core, start, count, order, merged):
        self.group, self.core, self.start, self.count = group, core, start, count
        self.order, self.merged = order, merged


def plan(groups, rows, Z):
    pairs = []
    for g in range(groups):
        if rows % 32:
            pairs.append([(g, tc, 0, rows) for tc in range(2)])
            continue
        for tc in range(2):
            small = rows % 64 == 0 and (g == groups - 1 or (g, tc) == (1, 1))
            parts = 4 if small else 2
            for i in range(0, parts, 2):
                pairs.append([(g, tc, (i + h) * (rows // parts), rows // parts) for h in range(2)])
    largest = max(pair[0][3] for pair in pairs)
    found = []
    for n, pair in enumerate(pairs):
        turned = n in TURNED and len(pairs) > 2 * len(TURNED)
        way = ("zxy", "zyx") if turned else ("xyz", "yxz")
        merged = Z == 4 and not turned and pair[0][3] == largest
        found.append([Unit(*part, order, merged) for part, order in zip(pair, way)])
    return found


def unit_sizes(unit, Z, X):
    return {
        "xyz": (2 * Z, Z, 6 if unit.merged else Z),
        "yxz": (Z, Z * X, 6 if unit.merged else Z),
        "zxy": (2, 1, Z * 2 * X),
        "zyx": (1, X, Z * 2 * X),
    }[unit.order]


def step_kernel(
    cfg, wave_hbm, targets_hbm, sizes_hbm, ids_hbm, coefs_hbm, left_hbm, right_hbm, out_ref,
    targets_ref, sizes_ref, ids_ref, coefs_ref,
    wave_ref, wbuf, lbuf, rbuf, acc, first_acc, left, own, psend, precv, weight_ref, wother, fsend, frecv, totals,
    xs, xr, ys, yr, zs, zr, load_sem, send_sem, recv_sem, pair_sem, gat_s, gat_r, relay_s,
):
    Z, X, T, K, rows, block, groups, pairs = cfg
    units = [unit for pair in pairs for unit in pair]
    offsets, ends = [], [0, 0, 0]
    for unit in units:
        offsets.append(tuple(ends))
        ends = [end + size * unit.count for end, size in zip(ends, unit_sizes(unit, Z, X))]
    grain = min(unit.count for unit in units)
    half = block // 2
    pair, sector = lax.axis_index("pair"), lax.axis_index("sector")
    z, x = pair // X, lax.rem(pair, X)
    y, c = sector // 2, lax.rem(sector, 2)

    def dev(zz=None, xx=None, yy=None, cc=None):
        zz, xx = z if zz is None else zz, x if xx is None else xx
        yy, cc = y if yy is None else yy, c if cc is None else cc
        return (zz * X + xx, yy * 2 + cc)

    x_dev, y_dev, c_dev = dev(xx=1 - x), dev(yy=1 - y), dev(cc=1 - c)
    up_dev, dn_dev = dev(zz=z + 1), dev(zz=z - 1)

    def loop(count, f):
        def one(i, carry):
            f(i)
            return carry

        lax.fori_loop(0, count, one, 0)

    has_up, has_dn = z + 1 < Z, z >= 1
    nested = Z == 4 and rows % LANES == 0
    pieces = PIECES
    width = block // pieces
    late = range(pieces // 2, pieces) if nested else ()

    left_loads = [pltpu.make_async_copy(left_hbm.at[k], lbuf.at[k], load_sem.at[0]) for k in range(K)]
    right_loads = []
    for k in range(K):
        for g in range(groups):
            for j in range(2):
                at = pl.multiple_of((1 - c if j == 0 else c) * half + g * LANES, LANES)
                right_loads.append(
                    pltpu.make_async_copy(
                        right_hbm.at[k, pl.ds(at, LANES)], rbuf.at[k, g, j],
                        load_sem.at[1],
                    )
                )

    barrier = pltpu.get_barrier_semaphore()
    for other in (x_dev, y_dev, c_dev):
        pl.semaphore_signal(barrier, inc=1, device_id=other, device_id_type=MESH)

    wave_load = pltpu.make_async_copy(wave_hbm, wave_ref, load_sem.at[2])
    wave_load.start()
    small_loads = [
        pltpu.make_async_copy(src, dst, load_sem.at[3 + i])
        for i, (src, dst) in enumerate(
            ((targets_hbm, targets_ref), (sizes_hbm, sizes_ref), (ids_hbm, ids_ref), (coefs_hbm, coefs_ref))
        )
    ]
    for copy in small_loads:
        copy.start()

    @pl.when(has_up)
    def _():
        pl.semaphore_signal(barrier, inc=1, device_id=up_dev, device_id_type=MESH)

    @pl.when(has_dn)
    def _():
        pl.semaphore_signal(barrier, inc=1, device_id=dn_dev, device_id_type=MESH)

    def rows_of(n, axis, index):
        count = units[n].count
        return pl.ds(pl.multiple_of(offsets[n][axis] + index * count, grain), count)

    def z_index(n, zz, ty=0, xx=0):
        return zz if units[n].order[2] == "z" else (zz * 2 + ty) * X + xx

    for n, unit in enumerate(units):
        if unit.merged:
            zr[pl.ds(offsets[n][2] + 2 * unit.count, 2 * unit.count), :] = jnp.zeros((2 * unit.count, LANES), BF16)
            continue
        size = unit_sizes(unit, Z, X)[2] // Z * unit.count
        zr[pl.ds(pl.multiple_of(offsets[n][2] + z * size, grain), size), :] = jnp.zeros((size, LANES), BF16)
    for copy in left_loads:
        copy.start()
    for copy in small_loads:
        copy.wait()
    for k in range(K):
        factor = coefs_ref[ids_ref[k]]
        for t in range(T):
            chosen = jnp.where(targets_ref[k] == t, factor, 0.0)
            weight_ref[k * T + t] = jnp.full((8, LANES), chosen, F32)
    size = sizes_ref[sector]

    def used(column, start=0, count=rows):
        row_ids = pair * rows + start + lax.broadcasted_iota(jnp.int32, (count, LANES), 0)
        lane_ids = column + lax.broadcasted_iota(jnp.int32, (count, LANES), 1)
        return ((row_ids < size) & (lane_ids < size)).astype(F32)

    wave_load.wait()
    for at in range(0, block, LANES):
        value = wave_ref[:, at : at + LANES].astype(F32) * used(at)
        p = at // width
        where = (x, p, z) if nested else (p, z, x)
        wbuf[(*where, slice(None), slice(at - p * width, at - p * width + LANES))] = value.astype(BF16)
    pl.semaphore_wait(barrier, 3 + has_up.astype(jnp.int32) + has_dn.astype(jnp.int32))

    def remote(src, dst, ss, rs, device):
        return pltpu.make_async_remote_copy(
            src_ref=src, dst_ref=dst, send_sem=ss, recv_sem=rs, device_id=device, device_id_type=MESH
        )

    def block_at(q, xx, p):
        return wbuf.at[(xx, p, q) if nested else (p, q, xx)]

    def hop(q, way, p):
        device = (up_dev, dn_dev, x_dev)[way]
        return remote(block_at(q, x, p), block_at(q, x, p), gat_s.at[way], gat_r.at[q, x, p], device)

    def arrival(q, xx, p):
        return remote(block_at(q, xx, p), block_at(q, xx, p), gat_s.at[2], gat_r.at[q, xx, p], x_dev)

    def skips_x(q, p):
        if p not in late:
            return jnp.bool_(False)
        return q == jnp.where(z == 0, 2, jnp.where(z == 1, 0, jnp.where(z == 2, 3, 1)))

    def relay(q, way):
        for p in late:
            block_there = block_at(q, 1 - x, p)
            remote(block_there, block_there, relay_s.at[0], gat_r.at[q, 1 - x, p], (up_dev, dn_dev)[way]).start()

    def relay_when(where, q, way):
        @pl.when(z == where)
        def _():
            relay(q, way)

    def pass_on(q, ways, p):
        if 0 in ways:
            @pl.when(has_up)
            def _():
                hop(q, 0, p).start()

        if 1 in ways:
            @pl.when(has_dn)
            def _():
                hop(q, 1, p).start()

        @pl.when(jnp.logical_not(skips_x(q, p)))
        def _():
            hop(q, 2, p).start()

    for p in range(pieces):
        pass_on(z, (0, 1), p)
    weights_copy = remote(weight_ref, wother, send_sem.at[0], recv_sem.at[0], c_dev)
    weights_copy.start()
    for copy in right_loads:
        copy.start()

    tile = min(ROW_TILE, block)
    tiles = block // tile

    def multiply(j, xx, ps, stage, ks=tuple(range(K))):
        def one(i, carry):
            k, at = ks[0] + i // tiles, pl.multiple_of(lax.rem(i, tiles) * tile, tile)
            sides = [
                lbuf[k, pl.ds(at, tile), pl.ds(pl.multiple_of(((2 * j + n) * X + xx) * rows, rows), rows)]
                for n in range(2)
            ]
            both = jnp.concatenate(sides, axis=1)
            for p in ps:
                product = jnp.dot(
                    both, wbuf[xx, p, pl.ds(2 * j, 2)].reshape(2 * rows, width), preferred_element_type=F32
                )
                if stage == "first":
                    acc[k, p, pl.ds(at, tile), :] = product
                elif stage == "middle":
                    acc[k, p, pl.ds(at, tile), :] += product
                else:
                    left[k, pl.ds(at, tile), pl.ds(p * width, width)] = (
                        acc[k, p, pl.ds(at, tile), :] + product
                    ).astype(BF16)
            return carry

        lax.fori_loop(0, len(ks) * tiles, one, 0)

    def split_term(g, k, at, term):
        psend[g, k, pl.ds(at, tile), :] = term[:, :LANES].astype(BF16)
        own[g, k, pl.ds(at, tile), :] = term[:, LANES:]

    def core_copy(g, k):
        return remote(psend.at[g, k], precv.at[g, k], send_sem.at[1], recv_sem.at[1 + g], c_dev)

    def first_second(h):
        cols = pl.ds(h * block // 2, block // 2)

        def one(i, carry):
            at = pl.multiple_of(i * tile, tile)
            for k in range(K):
                term = lax.dot_general(
                    left[k, pl.ds(at, tile), cols], rbuf[k, 0, :, :, cols].reshape(2 * LANES, block // 2),
                    (((1,), (1,)), ((), ())), preferred_element_type=F32,
                )
                if h == 0:
                    first_acc[k, pl.ds(at, tile), :] = term
                else:
                    split_term(0, k, at, first_acc[k, pl.ds(at, tile), :] + term)
            return carry

        lax.fori_loop(0, tiles, one, 0)
        if h == 1:
            for k in range(K):
                core_copy(0, k).start()

    def forward(d, p):
        lo, hi = z - d, z + d

        @pl.when(lo >= 0)
        def _():
            arrival(lo, x, p).wait_recv()
            pass_on(lo, (0,), p)

        @pl.when(hi < Z)
        def _():
            arrival(hi, x, p).wait_recv()
            pass_on(hi, (1,), p)

    def mirrored(q):
        for p in range(pieces):
            arrival(q, 1 - x, p).wait_recv()

    pltpu.make_async_copy(lbuf, lbuf, load_sem.at[0]).wait()
    if nested:
        near = z // 2
        far = 1 - near
        far_first = jnp.where(near == 0, 2, 1)
        for p in range(pieces):
            forward(1, p)
        mirrored(z)
        relay_when(0, 0, 0)
        relay_when(3, 3, 1)
        every = tuple(range(pieces))
        halves = every[: pieces // 2], every[pieces // 2 :]
        multiply(near, x, every, "first")
        for p in every:
            forward(2, p)
        mirrored(4 * near + 1 - z)
        for k in range(K):
            multiply(near, 1 - x, every, "middle", (k,))
            if k < 2:
                for p in halves[0][k :: 2]:
                    forward(3, p)
        multiply(far, x, halves[0], "middle")
        for p in halves[1]:
            forward(3, p)
        multiply(far, x, halves[1], "middle")
        inner = (z == 1) | (z == 2)

        @pl.when(inner)
        def _():
            mirrored(far_first)

        relay_when(1, 2, 1)
        relay_when(2, 1, 0)
        pltpu.make_async_copy(rbuf, rbuf, load_sem.at[1]).wait()
        for h in range(2):
            @pl.when(jnp.logical_not(inner))
            def _(h=h):
                for p in halves[h]:
                    arrival(far_first, 1 - x, p).wait_recv()

            for p in halves[h]:
                arrival(4 * far + 1 - far_first, 1 - x, p).wait_recv()
            multiply(far, 1 - x, halves[h], "last")
            first_second(h)
    else:
        def forward_all(d, carry):
            for p in range(pieces):
                forward(d, p)
            return carry

        def mirrored_all(q, carry):
            mirrored(q)
            return carry

        def whole_left(i, carry):
            k, at = i // tiles, pl.multiple_of(lax.rem(i, tiles) * tile, tile)
            for p in range(pieces):
                value = jnp.dot(
                    lbuf[k, pl.ds(at, tile), :], wbuf[p].reshape(block, width), preferred_element_type=F32
                )
                left[k, pl.ds(at, tile), pl.ds(p * width, width)] = value.astype(BF16)
            return carry

        lax.fori_loop(1, Z, forward_all, 0)
        lax.fori_loop(0, Z, mirrored_all, 0)
        lax.fori_loop(0, K * tiles, whole_left, 0)
        pltpu.make_async_copy(rbuf, rbuf, load_sem.at[1]).wait()

    def core_arrival(g):
        return remote(psend.at[g], precv.at[g], send_sem.at[1], recv_sem.at[1 + g], c_dev)

    def second(g):
        def one(i, carry):
            at = pl.multiple_of(i * tile, tile)
            for k in range(K):
                term = lax.dot_general(
                    left[k, pl.ds(at, tile), :], rbuf[k, g].reshape(2 * LANES, block),
                    (((1,), (1,)), ((), ())), preferred_element_type=F32,
                )
                split_term(g, k, at, term)
            return carry

        lax.fori_loop(0, tiles, one, 0)
        for k in range(K):
            core_copy(g, k).start()

    def chip_sum(n, ty, zz, xx):
        unit = units[n]
        at = pl.ds(pl.multiple_of((zz * X + xx) * rows + unit.start, unit.count), unit.count)
        t = ty * 2 + unit.core
        total = None
        for k in range(K):
            mine = own[unit.group, k, at, :] * weight_ref[k * T + t, 0:1, :]
            theirs = precv[unit.group, k, at, :].astype(F32) * wother[k * T + t, 0:1, :]
            total = mine + theirs if total is None else total + mine + theirs
        return total

    def put_x(n, index, value):
        xs[rows_of(n, 0, index), :] = value.astype(BF16)

    def put_y(n, index, value):
        ys[rows_of(n, 1, index), :] = value.astype(BF16)

    def put_z(n, index, value):
        zs[rows_of(n, 2, index), :] = value.astype(BF16)

    def from_x(n, index):
        return xr[rows_of(n, 0, index), :].astype(F32)

    def from_y(n, index):
        return yr[rows_of(n, 1, index), :].astype(F32)

    def from_z(n, index):
        return zr[rows_of(n, 2, index), :].astype(F32)

    def step_copy(n, letter, slot):
        axis = "xy".index(letter)
        s, r = ((xs, xr), (ys, yr))[axis]
        span = pl.ds(offsets[n][axis], unit_sizes(units[n], Z, X)[axis] * units[n].count)
        device = (x_dev, y_dev)[axis]
        return remote(s.at[span], r.at[span], send_sem.at[2 + axis], pair_sem.at[pair_of[n], slot], device)

    def z_span(n, zz):
        size = units[n].count * (1 if units[n].merged else unit_sizes(units[n], Z, X)[2] // Z)
        return pl.ds(pl.multiple_of(offsets[n][2] + zz * size, grain), size)

    def line_copy(n, zz):
        sem = pair_sem.at[pair_of[n], 2 if units[n].order[2] == "z" else 0]
        return remote(zs.at[z_span(n, zz)], zr.at[z_span(n, z)], send_sem.at[4], sem, dev(zz=zz))

    def merged_copy(n, mine, there, zz, slot):
        return remote(
            zs.at[z_span(n, mine)], zr.at[z_span(n, there)], send_sem.at[4], pair_sem.at[pair_of[n], slot], dev(zz=zz)
        )

    def wait_rows(sem, count):
        if count:
            pltpu.make_async_copy(zs.at[pl.ds(0, count)], zs.at[pl.ds(0, count)], sem).wait()

    def wait_pair(i, slot):
        count = 0
        for n in numbers[i]:
            unit, sizes = units[n], unit_sizes(units[n], Z, X)
            if unit.merged and slot >= 2:
                count += 2 * unit.count
            elif unit.order[slot] == "z":
                count += sizes[2] // Z * (Z - 1) * unit.count
            else:
                count += sizes["xy".index(unit.order[slot])] * unit.count
        wait_rows(pair_sem.at[i, slot], count)

    at_end = (z == 0) | (z == Z - 1)
    buddy = z + 1 - 2 * lax.rem(z, 2)
    far_halves = ((2, 2 - z // 2), (3, 3 - 3 * (z // 2)))

    def others(f):
        loop(Z - 1, lambda j: f(lax.rem(z + 1 + j, Z)))

    def send(n):
        order = units[n].order
        if order == "xyz":
            def one(zz):
                for ty in range(2):
                    put_x(n, ty * Z + zz, chip_sum(n, ty, zz, 1 - x))

            loop(Z, one)
            step_copy(n, "x", 0).start()
        elif order == "yxz":
            def one(zz):
                for xx in range(X):
                    put_y(n, zz * X + xx, chip_sum(n, 1 - y, zz, xx))

            loop(Z, one)
            step_copy(n, "y", 0).start()
        else:
            def one(zz):
                for ty in range(2):
                    for xx in range(X):
                        put_z(n, z_index(n, zz, ty, xx), chip_sum(n, ty, zz, xx))
                line_copy(n, zz).start()

            others(one)

    def line_sum(n, value, ty=0, xx=0):
        if Z <= 8:
            for zz in range(Z):
                value = value + from_z(n, z_index(n, zz, ty, xx))
            return value
        return lax.fori_loop(0, Z, lambda zz, v: v + from_z(n, z_index(n, zz, ty, xx)), value)

    def summed(n, ty, xx):
        return line_sum(n, chip_sum(n, ty, z, xx), ty, xx)

    def send_again(n):
        order = units[n].order
        if order == "xyz":
            def one(zz):
                put_y(n, zz, chip_sum(n, 1 - y, zz, x) + from_x(n, (1 - y) * Z + zz))

            loop(Z, one)
        elif order == "yxz":
            def one(zz):
                put_x(n, zz, chip_sum(n, y, zz, 1 - x) + from_y(n, zz * X + 1 - x))

            loop(Z, one)
        else:
            for j in range(2):
                if order == "zxy":
                    put_x(n, j, summed(n, j, 1 - x))
                else:
                    put_y(n, j, summed(n, 1 - y, j))
        step_copy(n, order[1], 1).start()

    def plane_sum(n, zz):
        value = chip_sum(n, y, zz, x)
        if units[n].order == "xyz":
            return value + from_x(n, y * Z + zz) + from_y(n, zz)
        return value + from_y(n, zz * X + x) + from_x(n, zz)

    def send_last(n):
        order = units[n].order
        if units[n].merged:
            put_z(n, 0, plane_sum(n, buddy))
            for slot, zz in far_halves:
                put_z(n, slot, plane_sum(n, zz))

            @pl.when(at_end)
            def _():
                for slot, _ in far_halves:
                    merged_copy(n, slot, slot, buddy, 3).start()

            merged_copy(n, 0, 0, buddy, 2).start()
        elif order[2] == "z":
            def one(zz):
                put_z(n, zz, plane_sum(n, zz))
                line_copy(n, zz).start()

            others(one)
        elif order == "zxy":
            put_y(n, 0, summed(n, 1 - y, x) + from_x(n, 1 - y))
            step_copy(n, "y", 2).start()
        else:
            put_x(n, 0, summed(n, y, 1 - x) + from_y(n, 1 - x))
            step_copy(n, "x", 2).start()

    def merge(i):
        if not units[numbers[i][0]].merged:
            return

        @pl.when(jnp.logical_not(at_end))
        def _():
            wait_pair(i, 3)

        for n in numbers[i]:
            for slot, zz in far_halves:
                put_z(n, slot + 2, plane_sum(n, zz) + from_z(n, slot))

            @pl.when(jnp.logical_not(at_end))
            def _(n=n):
                for slot, zz in far_halves:
                    merged_copy(n, slot + 2, 1, zz, 2).start()

    def total(n):
        order = units[n].order
        if units[n].merged:
            return plane_sum(n, z) + from_z(n, 0) + from_z(n, 1)
        if order[2] == "z":
            return line_sum(n, plane_sum(n, z))
        if order == "zxy":
            return summed(n, y, x) + from_x(n, y) + from_y(n, 0)
        return summed(n, y, x) + from_y(n, x) + from_x(n, 0)

    def final_copy(g):
        return remote(fsend.at[g], frecv.at[g], send_sem.at[5], recv_sem.at[1 + groups + g], c_dev)

    numbers, pair_of = [], {}
    for i, members in enumerate(pairs):
        numbers.append([units.index(unit) for unit in members])
        for n in numbers[i]:
            pair_of[n] = i

    def finish(g):
        at = pl.multiple_of(c * half + g * LANES, LANES)
        for i in range(len(pairs)):
            if units[numbers[i][0]].group == g:
                wait_pair(i, 2)
        for n, unit in enumerate(units):
            if unit.group == g:
                totals[unit.core, pl.ds(unit.start, unit.count), :] = total(n)
        one, two = totals[0], totals[1]
        out_ref[:, pl.ds(at, LANES)] = jnp.where(c == 0, one, two) * used(at)
        fsend[g] = jnp.where(c == 0, two, one)
        final_copy(g).start()

    def each(f, i):
        for n in numbers[i]:
            f(n)

    ready = set()

    def receive(g):
        if g not in ready:
            ready.add(g)
            core_arrival(g).wait_recv()

    queue = list(range(1 if nested else 0, groups))

    def compute(count):
        for _ in range(min(count, len(queue))):
            second(queue.pop(0))

    def start_pair(i):
        g = units[numbers[i][0]].group
        while queue and queue[0] <= g:
            compute(1)
        receive(g)
        each(send, i)

    turned = [i for i in range(len(pairs)) if units[numbers[i][0]].order[0] == "z"]
    plain = [i for i in range(len(pairs)) if i not in turned]
    steps = len(plain)
    done = set()
    compute(1 if nested else 2)
    weights_copy.wait_recv()
    for i in range(min(len(pairs), 4)):
        start_pair(i)
    compute(1)
    following = len([i for i in plain if i < 4])
    for j in range(steps):
        wait_pair(plain[j], 0)
        each(send_again, plain[j])
        while following < steps and following < j + 4:
            start_pair(plain[following])
            following += 1
            compute(1)
        if j == steps - 1:
            for i in turned:
                wait_pair(i, 0)
                each(send_again, i)
        if j >= 1:
            wait_pair(plain[j - 1], 1)
            each(send_last, plain[j - 1])
        if j >= MERGE_LAG:
            merge(plain[j - MERGE_LAG])
    wait_pair(plain[steps - 1], 1)
    each(send_last, plain[steps - 1])
    for j in range(max(0, steps - MERGE_LAG), steps):
        merge(plain[j])
    for i in turned:
        wait_pair(i, 1)
        each(send_last, i)
    for g in (*range(1, groups - 1), 0, groups - 1):
        if g not in done:
            done.add(g)
            finish(g)
    for g in range(groups):
        final_copy(g).wait_recv()
        at = pl.multiple_of((1 - c) * half + g * LANES, LANES)
        out_ref[:, pl.ds(at, LANES)] = frecv[g] * used(at)

    for v in range(Z):
        @pl.when(z == v)
        def _(v=v):
            for way, count in ((0, v + 1 if v + 1 < Z else 0), (1, Z - v if v else 0)):
                if count:
                    span = left.at[0, pl.ds(0, count * rows)]
                    pltpu.make_async_copy(span, span, gat_s.at[way]).wait()

    count = Z * rows - len(late) * rows // pieces
    flat = left.at[0, pl.ds(0, count)]
    pltpu.make_async_copy(flat, flat, gat_s.at[2]).wait()
    if late:
        flat = left.at[0, pl.ds(0, len(late) * rows // pieces)]
        pltpu.make_async_copy(flat, flat, relay_s.at[0]).wait()
    weights_copy.wait_send()
    pltpu.make_async_copy(psend, psend, send_sem.at[1]).wait()
    pltpu.make_async_copy(xs, xs, send_sem.at[2]).wait()
    pltpu.make_async_copy(ys, ys, send_sem.at[3]).wait()
    wait_rows(
        send_sem.at[4],
        sum(u.count * (3 if u.merged else unit_sizes(u, Z, X)[2] // Z * (Z - 1)) for u in units),
    )
    pltpu.make_async_copy(fsend, fsend, send_sem.at[5]).wait()


def body(wave, left_ops, right_ops, targets, sector_sizes, pair_ids, pair_coefficients):
    block = wave.shape[2]
    rows = wave.shape[1]
    K = left_ops.shape[0]
    T = sector_sizes.shape[0]
    X = 2
    Z = lax.axis_size("pair") // X
    groups = block // 2 // LANES
    pairs = plan(groups, rows, Z)
    heights = [0, 0, 0]
    for pair in pairs:
        for unit in pair:
            heights = [height + size * unit.count for height, size in zip(heights, unit_sizes(unit, Z, X))]
    dma = pltpu.SemaphoreType.DMA
    nested = Z == 4 and rows % LANES == 0
    width = block // PIECES
    hbm = pl.BlockSpec(memory_space=pltpu.HBM)
    operands = (
        wave[0], targets.reshape(-1), sector_sizes, pair_ids, pair_coefficients, left_ops[:, 0], right_ops[:, 0]
    )
    out = pl.pallas_call(
        functools.partial(step_kernel, (Z, X, T, K, rows, block, groups, pairs)),
        out_shape=jax.ShapeDtypeStruct((rows, block), F32),
        in_specs=[hbm] * 7,
        out_specs=pl.BlockSpec(memory_space=pltpu.VMEM),
        scratch_shapes=[
            *(pltpu.SMEM(a.shape, a.dtype) for a in operands[1:5]),
            pltpu.VMEM((rows, block), BF16),
            pltpu.VMEM((X, PIECES, Z, rows, width) if nested else (PIECES, Z, X, rows, width), BF16),
            pltpu.VMEM((K, block, block), BF16),
            pltpu.VMEM((K, groups, 2, LANES, block), BF16),
            pltpu.VMEM((K, PIECES, block, width) if nested else (8, LANES), F32),
            pltpu.VMEM((K, block, 2 * LANES) if nested else (8, LANES), F32),
            pltpu.VMEM((K, block, block), BF16),
            pltpu.VMEM((groups, K, block, LANES), F32),
            pltpu.VMEM((groups, K, block, LANES), BF16),
            pltpu.VMEM((groups, K, block, LANES), BF16),
            pltpu.VMEM((K * T, 8, LANES), F32),
            pltpu.VMEM((K * T, 8, LANES), F32),
            pltpu.VMEM((groups, rows, LANES), F32),
            pltpu.VMEM((groups, rows, LANES), F32),
            pltpu.VMEM((2, rows, LANES), F32),
            *(pltpu.VMEM((height, LANES), BF16) for height in heights for _ in range(2)),
            dma((7,)), dma((6,)), dma((1 + 2 * groups,)), dma((len(pairs), 4)),
            dma((3,)), dma((Z, X, PIECES)), dma((1,)),
        ],
        compiler_params=pltpu.CompilerParams(
            collective_id=0, has_side_effects=True, vmem_limit_bytes=VMEM_LIMIT
        ),
        name="sigma_step",
    )(*(pltpu.with_memory_space_constraint(a, pltpu.HBM) for a in operands))
    return out[None]


def solution(mesh):
    placed = (
        P("sector", "pair", None),
        P("pair", "sector", None, None),
        P("pair", "sector", None, None),
        P("pair", "sector"),
        P(),
        P("pair"),
        P(),
    )
    return jax.shard_map(
        body, mesh=mesh, in_specs=placed, out_specs=P("sector", "pair", None), check_vma=False
    )
```

```python
import functools

import jax
import jax.numpy as jnp
from jax import lax
from jax.experimental import pallas as pl
from jax.experimental.pallas import tpu as pltpu
from jax.sharding import PartitionSpec as P

MESH = pl.DeviceIdType.MESH
F32 = jnp.float32
BF16 = jnp.bfloat16
LANES = 128
ROW_TILE = 1024
PIECES = 4
VMEM_LIMIT = 48 * 1024 * 1024
TURNED = (1, 3, 4)
MERGE_LAG = 3


class Unit:
    def __init__(self, group, core, start, count, order, merged):
        self.group, self.core, self.start, self.count = group, core, start, count
        self.order, self.merged = order, merged


def plan(groups, rows, Z):
    pairs = []
    for g in range(groups):
        if rows % 32:
            pairs.append([(g, tc, 0, rows) for tc in range(2)])
            continue
        for tc in range(2):
            small = rows % 64 == 0 and (g == groups - 1 or (g, tc) == (1, 1))
            parts = 4 if small else 2
            for i in range(0, parts, 2):
                pairs.append([(g, tc, (i + h) * (rows // parts), rows // parts) for h in range(2)])
    largest = max(pair[0][3] for pair in pairs)
    found = []
    for n, pair in enumerate(pairs):
        turned = n in TURNED and len(pairs) > 2 * len(TURNED)
        way = ("zxy", "zyx") if turned else ("xyz", "yxz")
        merged = Z == 4 and not turned and pair[0][3] == largest
        found.append([Unit(*part, order, merged) for part, order in zip(pair, way)])
    return found


def unit_sizes(unit, Z, X):
    return {
        "xyz": (2 * Z, Z, 6 if unit.merged else Z),
        "yxz": (Z, Z * X, 6 if unit.merged else Z),
        "zxy": (2, 1, Z * 2 * X),
        "zyx": (1, X, Z * 2 * X),
    }[unit.order]


def step_kernel(
    cfg, wave_hbm, targets_hbm, sizes_hbm, ids_hbm, coefs_hbm, left_hbm, right_hbm, out_ref,
    targets_ref, sizes_ref, ids_ref, coefs_ref,
    wave_ref, wbuf, lbuf, rbuf, acc, first_acc, left, own, psend, precv, weight_ref, wother, fsend, frecv, totals,
    xs, xr, ys, yr, zs, zr, load_sem, send_sem, recv_sem, pair_sem, gat_s, gat_r, relay_s,
):
    Z, X, T, K, rows, block, groups, pairs = cfg
    units = [unit for pair in pairs for unit in pair]
    offsets, ends = [], [0, 0, 0]
    for unit in units:
        offsets.append(tuple(ends))
        ends = [end + size * unit.count for end, size in zip(ends, unit_sizes(unit, Z, X))]
    grain = min(unit.count for unit in units)
    half = block // 2
    pair, sector = lax.axis_index("pair"), lax.axis_index("sector")
    z, x = pair // X, lax.rem(pair, X)
    y, c = sector // 2, lax.rem(sector, 2)

    def dev(zz=None, xx=None, yy=None, cc=None):
        zz, xx = z if zz is None else zz, x if xx is None else xx
        yy, cc = y if yy is None else yy, c if cc is None else cc
        return (zz * X + xx, yy * 2 + cc)

    x_dev, y_dev, c_dev = dev(xx=1 - x), dev(yy=1 - y), dev(cc=1 - c)
    up_dev, dn_dev = dev(zz=z + 1), dev(zz=z - 1)

    def loop(count, f):
        def one(i, carry):
            f(i)
            return carry

        lax.fori_loop(0, count, one, 0)

    has_up, has_dn = z + 1 < Z, z >= 1
    nested = Z == 4 and rows % LANES == 0
    pieces = PIECES
    width = block // pieces
    late = range(pieces // 2, pieces) if nested else ()

    left_loads = [pltpu.make_async_copy(left_hbm.at[k], lbuf.at[k], load_sem.at[0]) for k in range(K)]
    right_loads = []
    for k in range(K):
        for g in range(groups):
            for j in range(2):
                at = pl.multiple_of((1 - c if j == 0 else c) * half + g * LANES, LANES)
                right_loads.append(
                    pltpu.make_async_copy(
                        right_hbm.at[k, pl.ds(at, LANES)], rbuf.at[k, g, j],
                        load_sem.at[1],
                    )
                )

    barrier = pltpu.get_barrier_semaphore()
    for other in (x_dev, y_dev, c_dev):
        pl.semaphore_signal(barrier, inc=1, device_id=other, device_id_type=MESH)

    wave_load = pltpu.make_async_copy(wave_hbm, wave_ref, load_sem.at[2])
    wave_load.start()
    small_loads = [
        pltpu.make_async_copy(src, dst, load_sem.at[3 + i])
        for i, (src, dst) in enumerate(
            ((targets_hbm, targets_ref), (sizes_hbm, sizes_ref), (ids_hbm, ids_ref), (coefs_hbm, coefs_ref))
        )
    ]
    for copy in small_loads:
        copy.start()

    @pl.when(has_up)
    def _():
        pl.semaphore_signal(barrier, inc=1, device_id=up_dev, device_id_type=MESH)

    @pl.when(has_dn)
    def _():
        pl.semaphore_signal(barrier, inc=1, device_id=dn_dev, device_id_type=MESH)

    def rows_of(n, axis, index):
        count = units[n].count
        return pl.ds(pl.multiple_of(offsets[n][axis] + index * count, grain), count)

    def z_index(n, zz, ty=0, xx=0):
        return zz if units[n].order[2] == "z" else (zz * 2 + ty) * X + xx

    for n, unit in enumerate(units):
        if unit.merged:
            zr[pl.ds(offsets[n][2] + 2 * unit.count, 2 * unit.count), :] = jnp.zeros((2 * unit.count, LANES), BF16)
            continue
        size = unit_sizes(unit, Z, X)[2] // Z * unit.count
        zr[pl.ds(pl.multiple_of(offsets[n][2] + z * size, grain), size), :] = jnp.zeros((size, LANES), BF16)
    for copy in left_loads:
        copy.start()
    for copy in small_loads:
        copy.wait()
    for k in range(K):
        factor = coefs_ref[ids_ref[k]]
        for t in range(T):
            chosen = jnp.where(targets_ref[k] == t, factor, 0.0)
            weight_ref[k * T + t] = jnp.full((8, LANES), chosen, F32)
    size = sizes_ref[sector]

    def used(column, start=0, count=rows):
        row_ids = pair * rows + start + lax.broadcasted_iota(jnp.int32, (count, LANES), 0)
        lane_ids = column + lax.broadcasted_iota(jnp.int32, (count, LANES), 1)
        return ((row_ids < size) & (lane_ids < size)).astype(F32)

    wave_load.wait()
    for at in range(0, block, LANES):
        value = wave_ref[:, at : at + LANES].astype(F32) * used(at)
        p = at // width
        where = (x, p, z) if nested else (p, z, x)
        wbuf[(*where, slice(None), slice(at - p * width, at - p * width + LANES))] = value.astype(BF16)
    pl.semaphore_wait(barrier, 3 + has_up.astype(jnp.int32) + has_dn.astype(jnp.int32))

    def remote(src, dst, ss, rs, device):
        return pltpu.make_async_remote_copy(
            src_ref=src, dst_ref=dst, send_sem=ss, recv_sem=rs, device_id=device, device_id_type=MESH
        )

    def block_at(q, xx, p):
        return wbuf.at[(xx, p, q) if nested else (p, q, xx)]

    def hop(q, way, p):
        device = (up_dev, dn_dev, x_dev)[way]
        return remote(block_at(q, x, p), block_at(q, x, p), gat_s.at[way], gat_r.at[q, x, p], device)

    def arrival(q, xx, p):
        return remote(block_at(q, xx, p), block_at(q, xx, p), gat_s.at[2], gat_r.at[q, xx, p], x_dev)

    def skips_x(q, p):
        if p not in late:
            return jnp.bool_(False)
        return q == jnp.where(z == 0, 2, jnp.where(z == 1, 0, jnp.where(z == 2, 3, 1)))

    def relay(q, way):
        for p in late:
            block_there = block_at(q, 1 - x, p)
            remote(block_there, block_there, relay_s.at[0], gat_r.at[q, 1 - x, p], (up_dev, dn_dev)[way]).start()

    def relay_when(where, q, way):
        @pl.when(z == where)
        def _():
            relay(q, way)

    def pass_on(q, ways, p):
        if 0 in ways:
            @pl.when(has_up)
            def _():
                hop(q, 0, p).start()

        if 1 in ways:
            @pl.when(has_dn)
            def _():
                hop(q, 1, p).start()

        @pl.when(jnp.logical_not(skips_x(q, p)))
        def _():
            hop(q, 2, p).start()

    for p in range(pieces):
        pass_on(z, (0, 1), p)
    weights_copy = remote(weight_ref, wother, send_sem.at[0], recv_sem.at[0], c_dev)
    weights_copy.start()
    for copy in right_loads:
        copy.start()

    tile = min(ROW_TILE, block)
    tiles = block // tile

    def multiply(j, xx, ps, stage, ks=tuple(range(K))):
        def one(i, carry):
            k, at = ks[0] + i // tiles, pl.multiple_of(lax.rem(i, tiles) * tile, tile)
            sides = [
                lbuf[k, pl.ds(at, tile), pl.ds(pl.multiple_of(((2 * j + n) * X + xx) * rows, rows), rows)]
                for n in range(2)
            ]
            both = jnp.concatenate(sides, axis=1)
            for p in ps:
                product = jnp.dot(
                    both, wbuf[xx, p, pl.ds(2 * j, 2)].reshape(2 * rows, width), preferred_element_type=F32
                )
                if stage == "first":
                    acc[k, p, pl.ds(at, tile), :] = product
                elif stage == "middle":
                    acc[k, p, pl.ds(at, tile), :] += product
                else:
                    left[k, pl.ds(at, tile), pl.ds(p * width, width)] = (
                        acc[k, p, pl.ds(at, tile), :] + product
                    ).astype(BF16)
            return carry

        lax.fori_loop(0, len(ks) * tiles, one, 0)

    def split_term(g, k, at, term):
        psend[g, k, pl.ds(at, tile), :] = term[:, :LANES].astype(BF16)
        own[g, k, pl.ds(at, tile), :] = term[:, LANES:]

    def core_copy(g, k):
        return remote(psend.at[g, k], precv.at[g, k], send_sem.at[1], recv_sem.at[1 + g], c_dev)

    def first_second(h):
        cols = pl.ds(h * block // 2, block // 2)

        def one(i, carry):
            at = pl.multiple_of(i * tile, tile)
            for k in range(K):
                term = lax.dot_general(
                    left[k, pl.ds(at, tile), cols], rbuf[k, 0, :, :, cols].reshape(2 * LANES, block // 2),
                    (((1,), (1,)), ((), ())), preferred_element_type=F32,
                )
                if h == 0:
                    first_acc[k, pl.ds(at, tile), :] = term
                else:
                    split_term(0, k, at, first_acc[k, pl.ds(at, tile), :] + term)
            return carry

        lax.fori_loop(0, tiles, one, 0)
        if h == 1:
            for k in range(K):
                core_copy(0, k).start()

    def forward(d, p):
        lo, hi = z - d, z + d

        @pl.when(lo >= 0)
        def _():
            arrival(lo, x, p).wait_recv()
            pass_on(lo, (0,), p)

        @pl.when(hi < Z)
        def _():
            arrival(hi, x, p).wait_recv()
            pass_on(hi, (1,), p)

    def mirrored(q):
        for p in range(pieces):
            arrival(q, 1 - x, p).wait_recv()

    pltpu.make_async_copy(lbuf, lbuf, load_sem.at[0]).wait()
    if nested:
        near = z // 2
        far = 1 - near
        far_first = jnp.where(near == 0, 2, 1)
        for p in range(pieces):
            forward(1, p)
        mirrored(z)
        relay_when(0, 0, 0)
        relay_when(3, 3, 1)
        every = tuple(range(pieces))
        halves = every[: pieces // 2], every[pieces // 2 :]
        multiply(near, x, every, "first")
        for p in every:
            forward(2, p)
        mirrored(4 * near + 1 - z)
        for k in range(K):
            multiply(near, 1 - x, every, "middle", (k,))
            if k < 2:
                for p in halves[0][k :: 2]:
                    forward(3, p)
        multiply(far, x, halves[0], "middle")
        for p in halves[1]:
            forward(3, p)
        multiply(far, x, halves[1], "middle")
        inner = (z == 1) | (z == 2)

        @pl.when(inner)
        def _():
            mirrored(far_first)

        relay_when(1, 2, 1)
        relay_when(2, 1, 0)
        pltpu.make_async_copy(rbuf, rbuf, load_sem.at[1]).wait()
        for h in range(2):
            @pl.when(jnp.logical_not(inner))
            def _(h=h):
                for p in halves[h]:
                    arrival(far_first, 1 - x, p).wait_recv()

            for p in halves[h]:
                arrival(4 * far + 1 - far_first, 1 - x, p).wait_recv()
            multiply(far, 1 - x, halves[h], "last")
            first_second(h)
    else:
        def forward_all(d, carry):
            for p in range(pieces):
                forward(d, p)
            return carry

        def mirrored_all(q, carry):
            mirrored(q)
            return carry

        def whole_left(i, carry):
            k, at = i // tiles, pl.multiple_of(lax.rem(i, tiles) * tile, tile)
            for p in range(pieces):
                value = jnp.dot(
                    lbuf[k, pl.ds(at, tile), :], wbuf[p].reshape(block, width), preferred_element_type=F32
                )
                left[k, pl.ds(at, tile), pl.ds(p * width, width)] = value.astype(BF16)
            return carry

        lax.fori_loop(1, Z, forward_all, 0)
        lax.fori_loop(0, Z, mirrored_all, 0)
        lax.fori_loop(0, K * tiles, whole_left, 0)
        pltpu.make_async_copy(rbuf, rbuf, load_sem.at[1]).wait()

    def core_arrival(g):
        return remote(psend.at[g], precv.at[g], send_sem.at[1], recv_sem.at[1 + g], c_dev)

    def second(g):
        def one(i, carry):
            at = pl.multiple_of(i * tile, tile)
            for k in range(K):
                term = lax.dot_general(
                    left[k, pl.ds(at, tile), :], rbuf[k, g].reshape(2 * LANES, block),
                    (((1,), (1,)), ((), ())), preferred_element_type=F32,
                )
                split_term(g, k, at, term)
            return carry

        lax.fori_loop(0, tiles, one, 0)
        for k in range(K):
            core_copy(g, k).start()

    def chip_sum(n, ty, zz, xx):
        unit = units[n]
        at = pl.ds(pl.multiple_of((zz * X + xx) * rows + unit.start, unit.count), unit.count)
        t = ty * 2 + unit.core
        total = None
        for k in range(K):
            mine = own[unit.group, k, at, :] * weight_ref[k * T + t, 0:1, :]
            theirs = precv[unit.group, k, at, :].astype(F32) * wother[k * T + t, 0:1, :]
            total = mine + theirs if total is None else total + mine + theirs
        return total

    def put_x(n, index, value):
        xs[rows_of(n, 0, index), :] = value.astype(BF16)

    def put_y(n, index, value):
        ys[rows_of(n, 1, index), :] = value.astype(BF16)

    def put_z(n, index, value):
        zs[rows_of(n, 2, index), :] = value.astype(BF16)

    def from_x(n, index):
        return xr[rows_of(n, 0, index), :].astype(F32)

    def from_y(n, index):
        return yr[rows_of(n, 1, index), :].astype(F32)

    def from_z(n, index):
        return zr[rows_of(n, 2, index), :].astype(F32)

    def step_copy(n, letter, slot):
        axis = "xy".index(letter)
        s, r = ((xs, xr), (ys, yr))[axis]
        span = pl.ds(offsets[n][axis], unit_sizes(units[n], Z, X)[axis] * units[n].count)
        device = (x_dev, y_dev)[axis]
        return remote(s.at[span], r.at[span], send_sem.at[2 + axis], pair_sem.at[pair_of[n], slot], device)

    def z_span(n, zz):
        size = units[n].count * (1 if units[n].merged else unit_sizes(units[n], Z, X)[2] // Z)
        return pl.ds(pl.multiple_of(offsets[n][2] + zz * size, grain), size)

    def line_copy(n, zz):
        sem = pair_sem.at[pair_of[n], 2 if units[n].order[2] == "z" else 0]
        return remote(zs.at[z_span(n, zz)], zr.at[z_span(n, z)], send_sem.at[4], sem, dev(zz=zz))

    def merged_copy(n, mine, there, zz, slot):
        return remote(
            zs.at[z_span(n, mine)], zr.at[z_span(n, there)], send_sem.at[4], pair_sem.at[pair_of[n], slot], dev(zz=zz)
        )

    def wait_rows(sem, count):
        if count:
            pltpu.make_async_copy(zs.at[pl.ds(0, count)], zs.at[pl.ds(0, count)], sem).wait()

    def wait_pair(i, slot):
        count = 0
        for n in numbers[i]:
            unit, sizes = units[n], unit_sizes(units[n], Z, X)
            if unit.merged and slot >= 2:
                count += 2 * unit.count
            elif unit.order[slot] == "z":
                count += sizes[2] // Z * (Z - 1) * unit.count
            else:
                count += sizes["xy".index(unit.order[slot])] * unit.count
        wait_rows(pair_sem.at[i, slot], count)

    at_end = (z == 0) | (z == Z - 1)
    buddy = z + 1 - 2 * lax.rem(z, 2)
    far_halves = ((2, 2 - z // 2), (3, 3 - 3 * (z // 2)))

    def others(f):
        loop(Z - 1, lambda j: f(lax.rem(z + 1 + j, Z)))

    def send(n):
        order = units[n].order
        if order == "xyz":
            def one(zz):
                for ty in range(2):
                    put_x(n, ty * Z + zz, chip_sum(n, ty, zz, 1 - x))

            loop(Z, one)
            step_copy(n, "x", 0).start()
        elif order == "yxz":
            def one(zz):
                for xx in range(X):
                    put_y(n, zz * X + xx, chip_sum(n, 1 - y, zz, xx))

            loop(Z, one)
            step_copy(n, "y", 0).start()
        else:
            def one(zz):
                for ty in range(2):
                    for xx in range(X):
                        put_z(n, z_index(n, zz, ty, xx), chip_sum(n, ty, zz, xx))
                line_copy(n, zz).start()

            others(one)

    def line_sum(n, value, ty=0, xx=0):
        if Z <= 8:
            for zz in range(Z):
                value = value + from_z(n, z_index(n, zz, ty, xx))
            return value
        return lax.fori_loop(0, Z, lambda zz, v: v + from_z(n, z_index(n, zz, ty, xx)), value)

    def summed(n, ty, xx):
        return line_sum(n, chip_sum(n, ty, z, xx), ty, xx)

    def send_again(n):
        order = units[n].order
        if order == "xyz":
            def one(zz):
                put_y(n, zz, chip_sum(n, 1 - y, zz, x) + from_x(n, (1 - y) * Z + zz))

            loop(Z, one)
        elif order == "yxz":
            def one(zz):
                put_x(n, zz, chip_sum(n, y, zz, 1 - x) + from_y(n, zz * X + 1 - x))

            loop(Z, one)
        else:
            for j in range(2):
                if order == "zxy":
                    put_x(n, j, summed(n, j, 1 - x))
                else:
                    put_y(n, j, summed(n, 1 - y, j))
        step_copy(n, order[1], 1).start()

    def plane_sum(n, zz):
        value = chip_sum(n, y, zz, x)
        if units[n].order == "xyz":
            return value + from_x(n, y * Z + zz) + from_y(n, zz)
        return value + from_y(n, zz * X + x) + from_x(n, zz)

    def send_last(n):
        order = units[n].order
        if units[n].merged:
            put_z(n, 0, plane_sum(n, buddy))
            for slot, zz in far_halves:
                put_z(n, slot, plane_sum(n, zz))

            @pl.when(at_end)
            def _():
                for slot, _ in far_halves:
                    merged_copy(n, slot, slot, buddy, 3).start()

            merged_copy(n, 0, 0, buddy, 2).start()
        elif order[2] == "z":
            def one(zz):
                put_z(n, zz, plane_sum(n, zz))
                line_copy(n, zz).start()

            others(one)
        elif order == "zxy":
            put_y(n, 0, summed(n, 1 - y, x) + from_x(n, 1 - y))
            step_copy(n, "y", 2).start()
        else:
            put_x(n, 0, summed(n, y, 1 - x) + from_y(n, 1 - x))
            step_copy(n, "x", 2).start()

    def merge(i):
        if not units[numbers[i][0]].merged:
            return

        @pl.when(jnp.logical_not(at_end))
        def _():
            wait_pair(i, 3)

        for n in numbers[i]:
            for slot, zz in far_halves:
                put_z(n, slot + 2, plane_sum(n, zz) + from_z(n, slot))

            @pl.when(jnp.logical_not(at_end))
            def _(n=n):
                for slot, zz in far_halves:
                    merged_copy(n, slot + 2, 1, zz, 2).start()

    def total(n):
        order = units[n].order
        if units[n].merged:
            return plane_sum(n, z) + from_z(n, 0) + from_z(n, 1)
        if order[2] == "z":
            return line_sum(n, plane_sum(n, z))
        if order == "zxy":
            return summed(n, y, x) + from_x(n, y) + from_y(n, 0)
        return summed(n, y, x) + from_y(n, x) + from_x(n, 0)

    def final_copy(g):
        return remote(fsend.at[g], frecv.at[g], send_sem.at[5], recv_sem.at[1 + groups + g], c_dev)

    numbers, pair_of = [], {}
    for i, members in enumerate(pairs):
        numbers.append([units.index(unit) for unit in members])
        for n in numbers[i]:
            pair_of[n] = i

    def finish(g):
        at = pl.multiple_of(c * half + g * LANES, LANES)
        for i in range(len(pairs)):
            if units[numbers[i][0]].group == g:
                wait_pair(i, 2)
        for n, unit in enumerate(units):
            if unit.group == g:
                totals[unit.core, pl.ds(unit.start, unit.count), :] = total(n)
        one, two = totals[0], totals[1]
        out_ref[:, pl.ds(at, LANES)] = jnp.where(c == 0, one, two) * used(at)
        fsend[g] = jnp.where(c == 0, two, one)
        final_copy(g).start()

    def each(f, i):
        for n in numbers[i]:
            f(n)

    ready = set()

    def receive(g):
        if g not in ready:
            ready.add(g)
            core_arrival(g).wait_recv()

    queue = list(range(1 if nested else 0, groups))

    def compute(count):
        for _ in range(min(count, len(queue))):
            second(queue.pop(0))

    def start_pair(i):
        g = units[numbers[i][0]].group
        while queue and queue[0] <= g:
            compute(1)
        receive(g)
        each(send, i)

    turned = [i for i in range(len(pairs)) if units[numbers[i][0]].order[0] == "z"]
    plain = [i for i in range(len(pairs)) if i not in turned]
    steps = len(plain)
    done = set()
    compute(0 if nested else 2)
    weights_copy.wait_recv()
    for i in range(min(len(pairs), 5)):
        start_pair(i)
    compute(1)
    following = len([i for i in plain if i < 5])
    for j in range(steps):
        wait_pair(plain[j], 0)
        each(send_again, plain[j])
        while following < steps and following < j + 3:
            start_pair(plain[following])
            following += 1
            compute(1)
        if j == steps - 1:
            for i in turned:
                wait_pair(i, 0)
                each(send_again, i)
        if j >= 1:
            wait_pair(plain[j - 1], 1)
            each(send_last, plain[j - 1])
        if j >= MERGE_LAG:
            merge(plain[j - MERGE_LAG])
    wait_pair(plain[steps - 1], 1)
    each(send_last, plain[steps - 1])
    for j in range(max(0, steps - MERGE_LAG), steps):
        merge(plain[j])
    for i in turned:
        wait_pair(i, 1)
        each(send_last, i)
    for g in (*range(1, groups - 1), 0, groups - 1):
        if g not in done:
            done.add(g)
            finish(g)
    for g in range(groups):
        final_copy(g).wait_recv()
        at = pl.multiple_of((1 - c) * half + g * LANES, LANES)
        out_ref[:, pl.ds(at, LANES)] = frecv[g] * used(at)

    for v in range(Z):
        @pl.when(z == v)
        def _(v=v):
            for way, count in ((0, v + 1 if v + 1 < Z else 0), (1, Z - v if v else 0)):
                if count:
                    span = left.at[0, pl.ds(0, count * rows)]
                    pltpu.make_async_copy(span, span, gat_s.at[way]).wait()

    count = Z * rows - len(late) * rows // pieces
    flat = left.at[0, pl.ds(0, count)]
    pltpu.make_async_copy(flat, flat, gat_s.at[2]).wait()
    if late:
        flat = left.at[0, pl.ds(0, len(late) * rows // pieces)]
        pltpu.make_async_copy(flat, flat, relay_s.at[0]).wait()
    weights_copy.wait_send()
    pltpu.make_async_copy(psend, psend, send_sem.at[1]).wait()
    pltpu.make_async_copy(xs, xs, send_sem.at[2]).wait()
    pltpu.make_async_copy(ys, ys, send_sem.at[3]).wait()
    wait_rows(
        send_sem.at[4],
        sum(u.count * (3 if u.merged else unit_sizes(u, Z, X)[2] // Z * (Z - 1)) for u in units),
    )
    pltpu.make_async_copy(fsend, fsend, send_sem.at[5]).wait()


def body(wave, left_ops, right_ops, targets, sector_sizes, pair_ids, pair_coefficients):
    block = wave.shape[2]
    rows = wave.shape[1]
    K = left_ops.shape[0]
    T = sector_sizes.shape[0]
    X = 2
    Z = lax.axis_size("pair") // X
    groups = block // 2 // LANES
    pairs = plan(groups, rows, Z)
    heights = [0, 0, 0]
    for pair in pairs:
        for unit in pair:
            heights = [height + size * unit.count for height, size in zip(heights, unit_sizes(unit, Z, X))]
    dma = pltpu.SemaphoreType.DMA
    nested = Z == 4 and rows % LANES == 0
    width = block // PIECES
    hbm = pl.BlockSpec(memory_space=pltpu.HBM)
    operands = (
        wave[0], targets.reshape(-1), sector_sizes, pair_ids, pair_coefficients, left_ops[:, 0], right_ops[:, 0]
    )
    out = pl.pallas_call(
        functools.partial(step_kernel, (Z, X, T, K, rows, block, groups, pairs)),
        out_shape=jax.ShapeDtypeStruct((rows, block), F32),
        in_specs=[hbm] * 7,
        out_specs=pl.BlockSpec(memory_space=pltpu.VMEM),
        scratch_shapes=[
            *(pltpu.SMEM(a.shape, a.dtype) for a in operands[1:5]),
            pltpu.VMEM((rows, block), BF16),
            pltpu.VMEM((X, PIECES, Z, rows, width) if nested else (PIECES, Z, X, rows, width), BF16),
            pltpu.VMEM((K, block, block), BF16),
            pltpu.VMEM((K, groups, 2, LANES, block), BF16),
            pltpu.VMEM((K, PIECES, block, width) if nested else (8, LANES), F32),
            pltpu.VMEM((K, block, 2 * LANES) if nested else (8, LANES), F32),
            pltpu.VMEM((K, block, block), BF16),
            pltpu.VMEM((groups, K, block, LANES), F32),
            pltpu.VMEM((groups, K, block, LANES), BF16),
            pltpu.VMEM((groups, K, block, LANES), BF16),
            pltpu.VMEM((K * T, 8, LANES), F32),
            pltpu.VMEM((K * T, 8, LANES), F32),
            pltpu.VMEM((groups, rows, LANES), F32),
            pltpu.VMEM((groups, rows, LANES), F32),
            pltpu.VMEM((2, rows, LANES), F32),
            *(pltpu.VMEM((height, LANES), BF16) for height in heights for _ in range(2)),
            dma((7,)), dma((6,)), dma((1 + 2 * groups,)), dma((len(pairs), 4)),
            dma((3,)), dma((Z, X, PIECES)), dma((1,)),
        ],
        compiler_params=pltpu.CompilerParams(
            collective_id=0, has_side_effects=True, vmem_limit_bytes=VMEM_LIMIT
        ),
        name="sigma_step",
    )(*(pltpu.with_memory_space_constraint(a, pltpu.HBM) for a in operands))
    return out[None]


def solution(mesh):
    placed = (
        P("sector", "pair", None),
        P("pair", "sector", None, None),
        P("pair", "sector", None, None),
        P("pair", "sector"),
        P(),
        P("pair"),
        P(),
    )
    return jax.shard_map(
        body, mesh=mesh, in_specs=placed, out_specs=P("sector", "pair", None), check_vma=False
    )
```
